768 devices in a mesh: dp: 12 (over z), fsdp: 64 (over y, x, core).
Axes of the slice: x: 4, y: 8, z: 12, core: 2. Of those that a mesh axis runs over, the one named last changes fastest.
Arguments:
- hidden: bfloat16 [196608, 4096], P(('dp', 'fsdp')), may hold values from -6 to 6
- queries: bfloat16 [196608, 2048], P(('dp', 'fsdp')), may hold values from -6 to 6
- keys: bfloat16 [196608, 512], P(('dp', 'fsdp')), may hold values from -6 to 6
- target: bfloat16 [196608, 2048], P(('dp', 'fsdp')), may hold values from -6 to 6
- lengths: int32 [768], P(('dp', 'fsdp')), may hold values from 64 to 256
- value_weight_frozen: bfloat16 [4096, 512], P('fsdp'), may hold values from -0.09375 to 0.09375
- adapter_down_map: float32 [4096, 64], P('fsdp'), may hold values from -0.09375 to 0.09375
- adapter_up_map: float32 [64, 512], replicated, may hold values from -0.75 to 0.75
- average_down_map: float32 [4096, 64], P('fsdp'), may hold values from -0.09375 to 0.09375
- average_up_map: float32 [64, 512], replicated, may hold values from -0.75 to 0.75
Outputs:
- down_map_gradient: float32 [4096, 64], P('fsdp')
- up_map_gradient: float32 [64, 512], replicated
- average_down_next: float32 [4096, 64], P('fsdp')
- average_up_next: float32 [64, 512], replicated
- loss: float32 [], replicated
The draws below stay inside these ranges and needn't reach their ends.
Inputs may be any that keep to these rules, and one draw needn't show every extreme that they name: `lengths`: slots at or past a sequence's length are padding.
All inputs are finite; a program needn't handle non-finite values.
Results may differ from the reference program's by a relative error of at most 0.0049.
Values may be sent and summed in bfloat16 or wider, within the bound.
No kernel may reach another device: no remote copies, remote signals or barrier semaphores. Data moves between devices by JAX's collectives and lax.ppermute only.
A program may use at most 64 MiB of HBM per device.

```python
import math
import jax
import jax.numpy as jnp
from jax import lax

MODEL_DIM = 4096
HEADS = 16
KEY_VALUE_HEADS = 4
HEAD_DIM = 128
ADAPTER_RANK = 64
TOK_DEV = 256
TOKENS = 196608
DEVICES = 768


def aligned_pair(key):
    base_seed = jax.random.fold_in(key, 7101)
    sign_seed, query_seed, strength_seed, noise_query, noise_keys = jax.random.split(base_seed, 5)
    seq_count = TOKENS // TOK_DEV
    group_size = HEADS // KEY_VALUE_HEADS
    query_field = jnp.clip(jax.random.normal(noise_query, (TOKENS, HEADS * HEAD_DIM), jnp.float32), -6.0, 6.0)
    key_field = jnp.clip(jax.random.normal(noise_keys, (TOKENS, KEY_VALUE_HEADS * HEAD_DIM), jnp.float32), -6.0, 6.0)
    lowest = 4.5
    signs = (2 * jax.random.randint(sign_seed, (seq_count, KEY_VALUE_HEADS, HEAD_DIM), 0, 2) - 1).astype(jnp.float32)
    key_strength = jax.random.uniform(strength_seed, (seq_count, KEY_VALUE_HEADS, 1), jnp.float32, lowest, 6.0)
    query_strength = jax.random.uniform(query_seed, (seq_count, 2, HEADS, 1), jnp.float32, lowest, 6.0)
    score_gap = 1.8 / (5.25 * math.sqrt(HEAD_DIM))
    key_rows = jnp.stack([key_strength * signs, (key_strength - score_gap) * signs], axis=1)
    query_signs = jnp.repeat(signs, group_size, axis=1)
    query_rows = query_strength * query_signs[:, None]
    query_field = query_field.reshape(seq_count, TOK_DEV, HEADS * HEAD_DIM)
    query_field = query_field.at[:, 2:4].set(query_rows.reshape(seq_count, 2, HEADS * HEAD_DIM))
    key_field = key_field.reshape(seq_count, TOK_DEV, KEY_VALUE_HEADS * HEAD_DIM)
    key_field = key_field.at[:, 0:2].set(key_rows.reshape(seq_count, 2, KEY_VALUE_HEADS * HEAD_DIM))
    return (query_field.reshape(TOKENS, HEADS * HEAD_DIM), key_field.reshape(TOKENS, KEY_VALUE_HEADS * HEAD_DIM))


def draw_queries(key, part):
    return aligned_pair(key)[0].astype(jnp.bfloat16)


def draw_keys(key, part):
    return aligned_pair(key)[1].astype(jnp.bfloat16)


def with_ends(array, rng, smallest, high):
    longest = array.shape.index(max(array.shape))
    spots = []
    for shift in (0, 1):
        where = [jax.random.randint(jax.random.fold_in(rng, axis), (), 0, length) for axis, length in enumerate(array.shape)]
        where[longest] = (where[longest] + shift) % array.shape[longest]
        spots.append(tuple(where))
    return array.at[spots[0]].set(smallest).at[spots[1]].set(high)


def block_levels(own_key, shape, cuts, smallest, top_value):
    level = 1.0
    for axis_at, shards_of in cuts:
        draws = jax.random.uniform(jax.random.fold_in(jax.random.fold_in(own_key, 6), axis_at), (shards_of,), jnp.float32, smallest / len(cuts), top_value / len(cuts))
        level = level * jnp.repeat(jnp.exp(draws), shape[axis_at] // shards_of).reshape((-1,) + (1,) * (len(shape) - 1 - axis_at))
    return level


def gaussian(rng, shape, scale, bound, pieces=(), kind=jnp.bfloat16):
    array = scale * jax.random.normal(rng, shape, jnp.float32)
    if pieces:
        array = array * block_levels(rng, shape, pieces, -0.22, 0.18)
    return jnp.clip(array, -bound, bound).astype(kind)


def setup_inputs(seed: int = 0) -> dict:
    streams_of = jax.random.split(jax.random.key(seed), 11)
    return {
        "hidden": gaussian(streams_of[0], (TOKENS, MODEL_DIM), 1.0, 6.0, ((0, 768),)),
        "queries": draw_queries(jax.random.fold_in(streams_of[10], 71), 0),
        "keys": draw_keys(jax.random.fold_in(streams_of[10], 71), 0),
        "target": gaussian(streams_of[3], (TOKENS, HEADS * HEAD_DIM), 1.0, 6.0, ((0, 768),)),
        "lengths": with_ends(jax.random.randint(streams_of[4], (DEVICES,), TOK_DEV // 4, TOK_DEV + 1), jax.random.fold_in(streams_of[4], 1), TOK_DEV // 4, TOK_DEV).astype(jnp.int32),
        "value_weight_frozen": gaussian(streams_of[5], (MODEL_DIM, KEY_VALUE_HEADS * HEAD_DIM), MODEL_DIM ** -0.5, 0.09375, ((0, 64),)),
        "adapter_down_map": gaussian(streams_of[6], (MODEL_DIM, ADAPTER_RANK), MODEL_DIM ** -0.5, 0.09375, ((0, 64),), jnp.float32),
        "adapter_up_map": gaussian(streams_of[7], (ADAPTER_RANK, KEY_VALUE_HEADS * HEAD_DIM), ADAPTER_RANK ** -0.5, 0.75, (), jnp.float32),
        "average_down_map": gaussian(streams_of[8], (MODEL_DIM, ADAPTER_RANK), MODEL_DIM ** -0.5, 0.09375, ((0, 64),), jnp.float32),
        "average_up_map": gaussian(streams_of[9], (ADAPTER_RANK, KEY_VALUE_HEADS * HEAD_DIM), ADAPTER_RANK ** -0.5, 0.75, (), jnp.float32),
    }


adapter_scale = 2.0
average_decay = 0.9
learning_rate = 1.0
masked_score = -1e+30

def per_sequence(items):
    queries, keys, value_outputs, target, seq_length = items
    tok_rows = queries.shape[0]
    group_size = HEADS // KEY_VALUE_HEADS
    position = jnp.arange(tok_rows, dtype=jnp.int32)
    allowed = (position[None, :] <= position[:, None]) & (position[None, :] < seq_length)
    q_heads = queries.reshape(tok_rows, HEADS, HEAD_DIM).astype(jnp.float32)
    k_heads = jnp.repeat(keys.reshape(tok_rows, KEY_VALUE_HEADS, HEAD_DIM), group_size, axis=1).astype(jnp.float32)
    v_heads = jnp.repeat(value_outputs.reshape(tok_rows, KEY_VALUE_HEADS, HEAD_DIM), group_size, axis=1).astype(jnp.float32)
    scores = jnp.einsum('thd,shd->hts', q_heads, k_heads) / math.sqrt(HEAD_DIM)
    scores = jnp.where(allowed[None], scores, masked_score)
    attn_probs = jax.nn.softmax(scores, axis=-1).astype(jnp.bfloat16)
    output = jnp.einsum('hts,shd->thd', attn_probs.astype(jnp.float32), v_heads).reshape(tok_rows, HEADS * HEAD_DIM)
    live_rows = (position < seq_length)[:, None]
    differ = jnp.where(live_rows, output - target.astype(jnp.float32), 0.0)
    loss_part = jnp.sum(differ * differ)
    cotangent = differ.astype(jnp.bfloat16).reshape(tok_rows, HEADS, HEAD_DIM).astype(jnp.float32)
    value_grad = jnp.einsum('hts,thd->shd', attn_probs.astype(jnp.float32), cotangent)
    value_grad = value_grad.reshape(tok_rows, KEY_VALUE_HEADS, group_size, HEAD_DIM).sum(axis=2).reshape(tok_rows, KEY_VALUE_HEADS * HEAD_DIM)
    return (value_grad.astype(jnp.bfloat16), loss_part)

def reference(hidden, queries, keys, target, lengths, value_weight_frozen, adapter_down_map, adapter_up_map, average_down_map, average_up_map):
    down_factor_slice = adapter_down_map.astype(jnp.bfloat16)
    up_factor_slice = adapter_up_map.astype(jnp.bfloat16)
    frozen_value_output = jnp.dot(hidden, value_weight_frozen, preferred_element_type=jnp.float32)
    adapter_hidden = jnp.dot(hidden, down_factor_slice, preferred_element_type=jnp.float32).astype(jnp.bfloat16)
    value_outputs = (frozen_value_output + adapter_scale * jnp.dot(adapter_hidden, up_factor_slice, preferred_element_type=jnp.float32)).astype(jnp.bfloat16)
    token_grand_count = jnp.sum(lengths).astype(jnp.float32)
    value_grad, loss_parts = lax.map(per_sequence, (queries.reshape(DEVICES, TOK_DEV, HEADS * HEAD_DIM), keys.reshape(DEVICES, TOK_DEV, KEY_VALUE_HEADS * HEAD_DIM), value_outputs.reshape(DEVICES, TOK_DEV, KEY_VALUE_HEADS * HEAD_DIM), target.reshape(DEVICES, TOK_DEV, HEADS * HEAD_DIM), lengths))
    value_grad = value_grad.reshape(DEVICES * TOK_DEV, KEY_VALUE_HEADS * HEAD_DIM)
    loss = jnp.sum(loss_parts) / (2.0 * token_grand_count)
    adapter_factor = adapter_scale / token_grand_count
    up_map_gradient = adapter_factor * jnp.dot(adapter_hidden.T, value_grad, preferred_element_type=jnp.float32)
    latent_grad = jnp.dot(value_grad, up_factor_slice.T, preferred_element_type=jnp.float32).astype(jnp.bfloat16)
    down_map_gradient = adapter_factor * jnp.dot(hidden.T, latent_grad, preferred_element_type=jnp.float32)
    average_down_next = average_decay * average_down_map + (1.0 - average_decay) * (adapter_down_map - learning_rate * down_map_gradient)
    average_up_next = average_decay * average_up_map + (1.0 - average_decay) * (adapter_up_map - learning_rate * up_map_gradient)
    return (down_map_gradient, up_map_gradient, average_down_next, average_up_next, loss)
```

```python
import math

import jax
import jax.numpy as jnp
from jax import lax
from jax.experimental import pallas as pl
from jax.experimental.pallas import tpu as pltpu
from jax.sharding import PartitionSpec as P

HEADS = 16
KEY_VALUE_HEADS = 4
HEAD_DIM = 128
GROUP = HEADS // KEY_VALUE_HEADS
TOK = 256
MODEL = 4096
RANK = 64
KV_WIDTH = KEY_VALUE_HEADS * HEAD_DIM

adapter_scale = 2.0
average_decay = 0.9
learning_rate = 1.0
masked_score = -1e30

PIECE_ROWS = 40
CHUNKS = 8


def nt(a, b):
    return lax.dot_general(a, b, (((1,), (1,)), ((), ())), preferred_element_type=jnp.float32)


def nn(a, b):
    return lax.dot_general(a, b, (((1,), (0,)), ((), ())), preferred_element_type=jnp.float32)


def probs_kernel(length_ref, q_ref, k_ref, p_ref, pt_ref):
    length = length_ref[0]
    keys = k_ref[...]
    row = lax.broadcasted_iota(jnp.int32, (TOK, TOK), 0)
    col = lax.broadcasted_iota(jnp.int32, (TOK, TOK), 1)
    allowed = (col <= row) & (col < length)
    for g in range(GROUP):
        scores = nt(q_ref[:, g * HEAD_DIM : (g + 1) * HEAD_DIM], keys) * (1.0 / math.sqrt(HEAD_DIM))
        scores = jnp.where(allowed, scores, masked_score)
        weights = jnp.exp(scores - jnp.max(scores, axis=-1, keepdims=True))
        probs = weights * (1.0 / jnp.sum(weights, axis=-1, keepdims=True))
        p_ref[0, g * TOK : (g + 1) * TOK, :] = probs.astype(jnp.bfloat16)
        pt_ref[0, :, g * TOK : (g + 1) * TOK] = jnp.transpose(probs).astype(jnp.bfloat16)


def attention_probs(lengths, queries, keys):
    shape = jax.ShapeDtypeStruct
    return pl.pallas_call(
        probs_kernel,
        grid=(KEY_VALUE_HEADS,),
        in_specs=[
            pl.BlockSpec(memory_space=pltpu.SMEM),
            pl.BlockSpec((TOK, GROUP * HEAD_DIM), lambda h: (0, h)),
            pl.BlockSpec((TOK, HEAD_DIM), lambda h: (0, h)),
        ],
        out_specs=[
            pl.BlockSpec((1, GROUP * TOK, TOK), lambda h: (h, 0, 0)),
            pl.BlockSpec((1, TOK, GROUP * TOK), lambda h: (h, 0, 0)),
        ],
        out_shape=[
            shape((KEY_VALUE_HEADS, GROUP * TOK, TOK), jnp.bfloat16),
            shape((KEY_VALUE_HEADS, TOK, GROUP * TOK), jnp.bfloat16),
        ],
        compiler_params=pltpu.CompilerParams(vmem_limit_bytes=16 * 2**20),
        cost_estimate=pl.CostEstimate(flops=2**31, bytes_accessed=6 * 2**20, transcendentals=2**20),
        name="probs",
    )(lengths, queries, keys)


def grads_kernel(
    facts_ref, hidden, own_hbm, other_hbm, probs, probs_t, target, up_ref, out_ref,
    weight, cot, value_grad, sems,
):
    length, core = facts_ref[0], facts_ref[1]
    columns, rows = own_hbm.shape[0], own_hbm.shape[1]
    step = MODEL // rows
    loads = []
    for c in range(rows):
        copies = []
        for x in range(columns):
            base = c * step + x * 2 * RANK
            for i, (source, side) in enumerate(((own_hbm, core), (other_hbm, 1 - core))):
                place = pl.ds(pl.multiple_of(base + side * RANK, RANK), RANK)
                copies.append(pltpu.make_async_copy(source.at[x, c], weight.at[place, :], sems.at[c, 2 * x + i]))
        loads.append(copies)
    for copies in loads:
        for copy in copies:
            copy.start()

    up = up_ref[...].astype(jnp.bfloat16)
    total = None
    for c in range(rows):
        for copy in loads[c]:
            copy.wait()
        part = nn(hidden[:, c * step : (c + 1) * step], weight[c * step : (c + 1) * step, :])
        total = part if total is None else total + part
    latent = total[:, KV_WIDTH:].astype(jnp.bfloat16)
    values = (total[:, :KV_WIDTH] + adapter_scale * nn(latent, up)).astype(jnp.bfloat16)

    live = lax.broadcasted_iota(jnp.int32, (TOK, HEAD_DIM), 0) < length
    squares = jnp.zeros((TOK, HEAD_DIM), jnp.float32)
    for k in range(KEY_VALUE_HEADS):
        output = nn(probs[k], values[:, k * HEAD_DIM : (k + 1) * HEAD_DIM])
        for g in range(GROUP):
            h = k * GROUP + g
            aim = target[:, h * HEAD_DIM : (h + 1) * HEAD_DIM].astype(jnp.float32)
            differ = jnp.where(live, output[g * TOK : (g + 1) * TOK, :] - aim, 0.0)
            squares = squares + differ * differ
            cot[g * TOK : (g + 1) * TOK, :] = differ.astype(jnp.bfloat16)
        value_grad[:, k * HEAD_DIM : (k + 1) * HEAD_DIM] = nn(probs_t[k], cot[...]).astype(jnp.bfloat16)

    grad = value_grad[...]
    latent_grad_t = nt(up, grad).astype(jnp.bfloat16)
    up_term = lax.dot_general(latent, grad, (((0,), (0,)), ((), ())), preferred_element_type=jnp.float32)

    lane = lax.broadcasted_iota(jnp.int32, (RANK // 2, HEAD_DIM), 1) < RANK
    for m in range(MODEL // 512):
        term = nn(latent_grad_t, hidden[:, m * 512 : (m + 1) * 512])
        for i in range(4):
            a = term[: RANK // 2, i * 128 : (i + 1) * 128]
            b = term[RANK // 2 :, i * 128 : (i + 1) * 128]
            even = jnp.where(lane, a, pltpu.roll(b, RANK, 1))
            odd = jnp.where(lane, pltpu.roll(a, RANK, 1), b)
            out_ref[m * 8 + 2 * i, :32, :] = even.astype(jnp.bfloat16)
            out_ref[m * 8 + 2 * i + 1, :32, :] = odd.astype(jnp.bfloat16)

    loss = jnp.sum(jnp.sum(squares, axis=0, keepdims=True), axis=1, keepdims=True)
    high = loss.astype(jnp.bfloat16).astype(jnp.float32)
    sub8 = lax.broadcasted_iota(jnp.int32, (8, HEAD_DIM), 0)
    lane8 = lax.broadcasted_iota(jnp.int32, (8, HEAD_DIM), 1)
    count = jnp.full((8, HEAD_DIM), length, jnp.int32).astype(jnp.float32)
    facts = jnp.where(lane8 == 0, high, jnp.where(lane8 == 1, loss - high, jnp.where(lane8 == 2, count, 0.0)))
    for q in range(8):
        for b in range(4):
            tile = up_term[8 * q : 8 * q + 8, b * 128 : (b + 1) * 128]
            out_ref[8 * q + b, 32:, :] = jnp.where(sub8 < 4, tile, facts).astype(jnp.bfloat16)
            out_ref[8 * q + 4 + b, 32:, :] = jnp.where(sub8 < 4, pltpu.roll(tile, 4, 0), facts).astype(jnp.bfloat16)


def gradient_pieces(facts, hidden, own, other, probs, probs_t, target, up_map):
    vmem = pl.BlockSpec(memory_space=pltpu.VMEM)
    hbm = pl.BlockSpec(memory_space=pltpu.HBM)
    width = own.shape[-1]
    return pl.pallas_call(
        grads_kernel,
        in_specs=[pl.BlockSpec(memory_space=pltpu.SMEM), vmem, hbm, hbm, vmem, vmem, vmem, vmem],
        out_specs=vmem,
        out_shape=jax.ShapeDtypeStruct((MODEL // RANK, PIECE_ROWS, HEAD_DIM), jnp.bfloat16),
        scratch_shapes=[
            pltpu.VMEM((MODEL, width), jnp.bfloat16),
            pltpu.VMEM((GROUP * TOK, HEAD_DIM), jnp.bfloat16),
            pltpu.VMEM((TOK, KV_WIDTH), jnp.bfloat16),
            pltpu.SemaphoreType.DMA((own.shape[1], 2 * own.shape[0])),
        ],
        compiler_params=pltpu.CompilerParams(vmem_limit_bytes=32 * 2**20),
        cost_estimate=pl.CostEstimate(flops=2**32, bytes_accessed=14 * 2**20, transcendentals=0),
        name="grads",
    )(facts, hidden, own, other, probs, probs_t, target, up_map)


def fold_kernel(pieces_ref, out_ref):
    total = jnp.sum(pieces_ref[...].astype(jnp.float32), axis=0)
    for d in range(out_ref.shape[0]):
        out_ref[d] = total


def fold(pieces, copies):
    return pl.pallas_call(
        fold_kernel,
        out_shape=jax.ShapeDtypeStruct((copies, PIECE_ROWS, HEAD_DIM), jnp.float32),
        name="fold",
    )(pieces)


def owner_kernel(pieces_ref, down_ref, average_ref, grad_ref, next_ref, up_ref, loss_ref):
    total = jnp.sum(pieces_ref[...], axis=0)
    count = total[36:37, 2:3]
    loss_ref[...] = (total[36:37, 0:1] + total[36:37, 1:2]) / (2.0 * count)
    factor = adapter_scale / count
    rows = jnp.concatenate([total[:32, :RANK], total[:32, RANK:]], axis=0)
    grad = jnp.transpose(rows) * factor
    grad_ref[...] = grad
    next_ref[...] = average_decay * average_ref[...] + (1.0 - average_decay) * (down_ref[...] - learning_rate * grad)
    up_ref[0] = total[32:36, :] * factor


def owner_update(pieces, down_map, average_down_map):
    shape = jax.ShapeDtypeStruct
    return pl.pallas_call(
        owner_kernel,
        out_shape=[
            shape((RANK, RANK), jnp.float32),
            shape((RANK, RANK), jnp.float32),
            shape((1, 4, HEAD_DIM), jnp.float32),
            shape((1, 1), jnp.float32),
        ],
        name="owner",
    )(pieces, down_map, average_down_map)


def second_kernel(pieces_ref, up_ref, average_ref, grad_ref, next_ref):
    for j in range(MODEL // RANK):
        q, b = divmod(j, 4)
        grad_ref[4 * q : 4 * q + 4, b * 128 : (b + 1) * 128] = pieces_ref[j]
    next_ref[...] = average_decay * average_ref[...] + (1.0 - average_decay) * (
        up_ref[...] - learning_rate * grad_ref[...]
    )


def second_update(pieces, up_map, average_up_map):
    shape = jax.ShapeDtypeStruct((RANK, KV_WIDTH), jnp.float32)
    return pl.pallas_call(second_kernel, out_shape=[shape, shape], name="second")(pieces, up_map, average_up_map)


def exchange(pieces, axis):
    return lax.all_to_all(pieces, axis, 0, 0, tiled=True)


def along_y(owners):
    return [list(range(k, owners, 8)) for k in range(8)]


def along_x(owners):
    return [[y * 8 + x * 2 + core for x in range(4)] for y in range(owners // 8) for core in range(2)]


def gathered(shard, groups):
    copies = jnp.broadcast_to(shard[None], (len(groups[0]), *shard.shape))
    return lax.all_to_all(copies, "fsdp", 0, 0, tiled=True, axis_index_groups=groups)


def per_device(
    hidden,
    queries,
    keys,
    target,
    lengths,
    value_weight_frozen,
    adapter_down_map,
    adapter_up_map,
    average_down_map,
    average_up_map,
):
    owners, replicas = lax.axis_size("fsdp"), lax.axis_size("dp")
    core = lax.axis_index("fsdp").astype(jnp.int32) % 2
    facts = jnp.stack([lengths[0], core])
    both = jnp.concatenate([value_weight_frozen, adapter_down_map.astype(jnp.bfloat16)], axis=1)
    own = gathered(gathered(both, along_y(owners)), along_x(owners))
    other = lax.ppermute(own, "fsdp", [(i, i ^ 1) for i in range(owners)])
    probs, probs_t = attention_probs(lengths, queries, keys)
    pieces = gradient_pieces(facts, hidden, own, other, probs, probs_t, target, adapter_up_map)
    summed = fold(exchange(pieces, "fsdp"), replicas)
    down_grad, average_down_next, up_piece, loss = owner_update(
        exchange(summed, "dp"), adapter_down_map, average_down_map
    )
    up_pieces = exchange(jnp.broadcast_to(up_piece, (owners, 4, HEAD_DIM)), "fsdp")
    up_grad, average_up_next = second_update(up_pieces, adapter_up_map, average_up_map)
    return (down_grad, up_grad, average_down_next, average_up_next, loss.reshape(()))


def solution(mesh):
    placed = (
        P(("dp", "fsdp"), None),
        P(("dp", "fsdp"), None),
        P(("dp", "fsdp"), None),
        P(("dp", "fsdp"), None),
        P(("dp", "fsdp")),
        P("fsdp", None),
        P("fsdp", None),
        P(),
        P("fsdp", None),
        P(),
    )
    return jax.shard_map(
        per_device,
        mesh=mesh,
        in_specs=placed,
        out_specs=(P("fsdp", None), P(), P("fsdp", None), P(), P()),
        check_vma=False,
    )
```

```python
import functools
import math

import jax
import jax.numpy as jnp
from jax import lax
from jax.experimental import pallas as pl
from jax.experimental.pallas import tpu as pltpu
from jax.sharding import PartitionSpec as P


HEADS = 16
KEY_VALUE_HEADS = 4
HEAD_DIM = 128
GROUP = HEADS // KEY_VALUE_HEADS
TOK = 256
MODEL = 4096
RANK = 64
KV_WIDTH = KEY_VALUE_HEADS * HEAD_DIM
WIDTH = KV_WIDTH + RANK

adapter_scale = 2.0
average_decay = 0.9
learning_rate = 1.0
masked_score = -1e30

PIECE_ROWS = 40
SMALL = pltpu.CompilerParams(vmem_limit_bytes=4 * 2**20)


def nt(a, b):
    return lax.dot_general(a, b, (((1,), (1,)), ((), ())), preferred_element_type=jnp.float32)


def nn(a, b):
    return lax.dot_general(a, b, (((1,), (0,)), ((), ())), preferred_element_type=jnp.float32)


def probs_kernel(length_ref, q_ref, k_ref, p_ref, pt_ref):
    length = length_ref[0]
    keys = k_ref[...]
    row = lax.broadcasted_iota(jnp.int32, (TOK, TOK), 0)
    col = lax.broadcasted_iota(jnp.int32, (TOK, TOK), 1)
    allowed = (col <= row) & (col < length)
    for g in range(GROUP):
        scores = nt(q_ref[:, g * HEAD_DIM : (g + 1) * HEAD_DIM], keys) * (1.0 / math.sqrt(HEAD_DIM))
        scores = jnp.where(allowed, scores, masked_score)
        weights = jnp.exp(scores - jnp.max(scores, axis=-1, keepdims=True))
        probs = weights * (1.0 / jnp.sum(weights, axis=-1, keepdims=True))
        p_ref[0, g * TOK : (g + 1) * TOK, :] = probs.astype(jnp.bfloat16)
        pt_ref[0, :, g * TOK : (g + 1) * TOK] = jnp.transpose(probs).astype(jnp.bfloat16)


def attention_probs(lengths, queries, keys):
    shape = jax.ShapeDtypeStruct
    return pl.pallas_call(
        probs_kernel,
        grid=(KEY_VALUE_HEADS,),
        in_specs=[
            pl.BlockSpec(memory_space=pltpu.SMEM),
            pl.BlockSpec((TOK, GROUP * HEAD_DIM), lambda h: (0, h)),
            pl.BlockSpec((TOK, HEAD_DIM), lambda h: (0, h)),
        ],
        out_specs=[
            pl.BlockSpec((1, GROUP * TOK, TOK), lambda h: (h, 0, 0)),
            pl.BlockSpec((1, TOK, GROUP * TOK), lambda h: (h, 0, 0)),
        ],
        out_shape=[
            shape((KEY_VALUE_HEADS, GROUP * TOK, TOK), jnp.bfloat16),
            shape((KEY_VALUE_HEADS, TOK, GROUP * TOK), jnp.bfloat16),
        ],
        compiler_params=pltpu.CompilerParams(vmem_limit_bytes=16 * 2**20),
        cost_estimate=pl.CostEstimate(flops=2**31, bytes_accessed=6 * 2**20, transcendentals=2**20),
        name="probs",
    )(lengths, queries, keys)


def pack_kernel(value_ref, down_ref, out_ref):
    down = down_ref[...].astype(jnp.bfloat16)
    for d in range(out_ref.shape[0]):
        out_ref[d, :, :KV_WIDTH] = value_ref[...]
        out_ref[d, :, KV_WIDTH:] = down


def packed_shard(value_rows, down_rows, copies):
    return pl.pallas_call(
        pack_kernel,
        out_shape=jax.ShapeDtypeStruct((copies, RANK, WIDTH), jnp.bfloat16),
        compiler_params=SMALL,
        name="pack",
    )(value_rows, down_rows)


def block_product(facts_ref, which, hidden, first, second, out):
    x = lax.rem(facts_ref[2] + (4 - which), 4)
    total = None
    for y in range(0, first.shape[0], 2):
        left, right = [], []
        for i in (y, y + 1):
            left.append(hidden[:, pl.ds(pl.multiple_of(i * 512 + x * 128, 128), 128)])
            right += [first[i], second[i]]
        part = nn(jnp.concatenate(left, axis=1), jnp.concatenate(right, axis=0))
        total = part if total is None else total + part
    out[...] = total


def in_core_order(facts_ref, own, other, run):
    @pl.when(facts_ref[1] == 0)
    def _():
        run(own, other)

    @pl.when(facts_ref[1] != 0)
    def _():
        run(other, own)


def partial_kernel(which, facts_ref, hidden, own, other, *rest):
    out = rest[-1]
    in_core_order(facts_ref, own, other, lambda a, b: block_product(facts_ref, which, hidden, a, b, out))
    if len(rest) > 1:
        out[...] += rest[0][...]


def partial_values(facts, hidden, own, other, which, before=None):
    vmem = pl.BlockSpec(memory_space=pltpu.VMEM)
    given = () if before is None else (before,)
    return pl.pallas_call(
        functools.partial(partial_kernel, which),
        in_specs=[pl.BlockSpec(memory_space=pltpu.SMEM)] + [vmem] * (3 + len(given)),
        out_specs=vmem,
        out_shape=jax.ShapeDtypeStruct((TOK, WIDTH), jnp.float32),
        compiler_params=pltpu.CompilerParams(vmem_limit_bytes=8 * 2**20),
        cost_estimate=pl.CostEstimate(flops=2**29, bytes_accessed=2**21, transcendentals=0),
        name="partial",
    )(facts, hidden, own, other, *given)


def grads_kernel(
    facts_ref, hidden, own, other, before, probs, probs_t, target, up_ref, out_ref, last, cot, value_grad,
):
    length = facts_ref[0]
    up = up_ref[...].astype(jnp.bfloat16)
    in_core_order(facts_ref, own, other, lambda a, b: block_product(facts_ref, 2, hidden, a, b, last))
    total = last[...] + before[...]
    latent = total[:, KV_WIDTH:].astype(jnp.bfloat16)
    values = (total[:, :KV_WIDTH] + adapter_scale * nn(latent, up)).astype(jnp.bfloat16)

    live = lax.broadcasted_iota(jnp.int32, (TOK, HEAD_DIM), 0) < length
    squares = jnp.zeros((TOK, HEAD_DIM), jnp.float32)
    for k in range(KEY_VALUE_HEADS):
        output = nn(probs[k], values[:, k * HEAD_DIM : (k + 1) * HEAD_DIM])
        for g in range(GROUP):
            h = k * GROUP + g
            aim = target[:, h * HEAD_DIM : (h + 1) * HEAD_DIM].astype(jnp.float32)
            differ = jnp.where(live, output[g * TOK : (g + 1) * TOK, :] - aim, 0.0)
            squares = squares + differ * differ
            cot[g * TOK : (g + 1) * TOK, :] = differ.astype(jnp.bfloat16)
        value_grad[:, k * HEAD_DIM : (k + 1) * HEAD_DIM] = nn(probs_t[k], cot[...]).astype(jnp.bfloat16)

    grad = value_grad[...]
    latent_grad_t = nt(up, grad).astype(jnp.bfloat16)
    up_term = lax.dot_general(latent, grad, (((0,), (0,)), ((), ())), preferred_element_type=jnp.float32)

    lane = lax.broadcasted_iota(jnp.int32, (RANK // 2, HEAD_DIM), 1) < RANK
    for m in range(MODEL // 512):
        term = nn(latent_grad_t, hidden[:, m * 512 : (m + 1) * 512])
        for i in range(4):
            a = term[: RANK // 2, i * 128 : (i + 1) * 128]
            b = term[RANK // 2 :, i * 128 : (i + 1) * 128]
            even = jnp.where(lane, a, pltpu.roll(b, RANK, 1))
            odd = jnp.where(lane, pltpu.roll(a, RANK, 1), b)
            out_ref[m * 8 + 2 * i, :32, :] = even.astype(jnp.bfloat16)
            out_ref[m * 8 + 2 * i + 1, :32, :] = odd.astype(jnp.bfloat16)

    loss = jnp.sum(jnp.sum(squares, axis=0, keepdims=True), axis=1, keepdims=True)
    high = loss.astype(jnp.bfloat16).astype(jnp.float32)
    sub8 = lax.broadcasted_iota(jnp.int32, (8, HEAD_DIM), 0)
    lane8 = lax.broadcasted_iota(jnp.int32, (8, HEAD_DIM), 1)
    count = jnp.full((8, HEAD_DIM), length, jnp.int32).astype(jnp.float32)
    facts = jnp.where(lane8 == 0, high, jnp.where(lane8 == 1, loss - high, jnp.where(lane8 == 2, count, 0.0)))
    for q in range(8):
        for b in range(4):
            tile = up_term[8 * q : 8 * q + 8, b * 128 : (b + 1) * 128]
            out_ref[8 * q + b, 32:, :] = jnp.where(sub8 < 4, tile, facts).astype(jnp.bfloat16)
            out_ref[8 * q + 4 + b, 32:, :] = jnp.where(sub8 < 4, pltpu.roll(tile, 4, 0), facts).astype(jnp.bfloat16)


def gradient_pieces(facts, hidden, own, other, before, probs, probs_t, target, up_map):
    vmem = pl.BlockSpec(memory_space=pltpu.VMEM)
    return pl.pallas_call(
        grads_kernel,
        in_specs=[pl.BlockSpec(memory_space=pltpu.SMEM)] + [vmem] * 8,
        out_specs=vmem,
        out_shape=jax.ShapeDtypeStruct((MODEL // RANK, PIECE_ROWS, HEAD_DIM), jnp.bfloat16),
        scratch_shapes=[
            pltpu.VMEM((TOK, WIDTH), jnp.float32),
            pltpu.VMEM((GROUP * TOK, HEAD_DIM), jnp.bfloat16),
            pltpu.VMEM((TOK, KV_WIDTH), jnp.bfloat16),
        ],
        compiler_params=pltpu.CompilerParams(vmem_limit_bytes=24 * 2**20),
        cost_estimate=pl.CostEstimate(flops=2**32, bytes_accessed=10 * 2**20, transcendentals=0),
        name="grads",
    )(facts, hidden, own, other, before, probs, probs_t, target, up_map)


def fold_kernel(pieces_ref, out_ref):
    total = jnp.sum(pieces_ref[...].astype(jnp.float32), axis=0)
    for d in range(out_ref.shape[0]):
        out_ref[d] = total


def fold(pieces, copies):
    return pl.pallas_call(
        fold_kernel,
        out_shape=jax.ShapeDtypeStruct((copies, PIECE_ROWS, HEAD_DIM), jnp.float32),
        compiler_params=SMALL,
        name="fold",
    )(pieces)


def owner_kernel(pieces_ref, down_ref, average_ref, grad_ref, next_ref, up_ref, loss_ref):
    total = jnp.sum(pieces_ref[...], axis=0)
    count = total[36:37, 2:3]
    loss_ref[...] = (total[36:37, 0:1] + total[36:37, 1:2]) / (2.0 * count)
    factor = adapter_scale / count
    rows = jnp.concatenate([total[:32, :RANK], total[:32, RANK:]], axis=0)
    grad = jnp.transpose(rows) * factor
    grad_ref[...] = grad
    next_ref[...] = average_decay * average_ref[...] + (1.0 - average_decay) * (down_ref[...] - learning_rate * grad)
    piece = total[32:36, :] * factor
    for d in range(up_ref.shape[0]):
        up_ref[d] = piece


def owner_update(pieces, down_map, average_down_map, copies):
    shape = jax.ShapeDtypeStruct
    return pl.pallas_call(
        owner_kernel,
        out_shape=[
            shape((RANK, RANK), jnp.float32),
            shape((RANK, RANK), jnp.float32),
            shape((copies, 4, HEAD_DIM), jnp.float32),
            shape((1, 1), jnp.float32),
        ],
        compiler_params=SMALL,
        name="owner",
    )(pieces, down_map, average_down_map)


def second_kernel(pieces_ref, up_ref, average_ref, grad_ref, next_ref):
    for j in range(MODEL // RANK):
        q, b = divmod(j, 4)
        grad_ref[4 * q : 4 * q + 4, b * 128 : (b + 1) * 128] = pieces_ref[j]
    next_ref[...] = average_decay * average_ref[...] + (1.0 - average_decay) * (
        up_ref[...] - learning_rate * grad_ref[...]
    )


def second_update(pieces, up_map, average_up_map):
    shape = jax.ShapeDtypeStruct((RANK, KV_WIDTH), jnp.float32)
    return pl.pallas_call(second_kernel, out_shape=[shape, shape], compiler_params=SMALL, name="second")(
        pieces, up_map, average_up_map
    )


def exchange(pieces, axis):
    return lax.all_to_all(pieces, axis, 0, 0, tiled=True)


def along_y(owners):
    return [list(range(k, owners, 8)) for k in range(8)]


def along_x(block, owners, shift):
    moved = [(i, i // 8 * 8 + (i + 2 * shift) % 8) for i in range(owners)]
    return lax.ppermute(block, "fsdp", moved)


def from_other_core(block, owners):
    return lax.ppermute(block, "fsdp", [(i, i ^ 1) for i in range(owners)])


def per_device(
    hidden,
    queries,
    keys,
    target,
    lengths,
    value_weight_frozen,
    adapter_down_map,
    adapter_up_map,
    average_down_map,
    average_up_map,
):
    owners, replicas = lax.axis_size("fsdp"), lax.axis_size("dp")
    place = lax.axis_index("fsdp").astype(jnp.int32)
    facts = jnp.stack([lengths[0], place & 1, (place >> 1) & 3])
    shards = packed_shard(value_weight_frozen, adapter_down_map, owners // 8)
    own = lax.all_to_all(shards, "fsdp", 0, 0, tiled=True, axis_index_groups=along_y(owners))
    blocks, others, total = [own], [], None
    for shift in (1, 2, 3):
        blocks.append(along_x(own, owners, shift))
    for shift in range(4):
        others.append(from_other_core(blocks[shift], owners))
    probs, probs_t = attention_probs(lengths, queries, keys)
    for shift in (0, 1, 3):
        total = partial_values(facts, hidden, blocks[shift], others[shift], shift, total)
    pieces = gradient_pieces(
        facts, hidden, blocks[2], others[2], total, probs, probs_t, target, adapter_up_map
    )
    summed = fold(exchange(pieces, "fsdp"), replicas)
    down_grad, average_down_next, up_piece, loss = owner_update(
        exchange(summed, "dp"), adapter_down_map, average_down_map, owners
    )
    up_grad, average_up_next = second_update(exchange(up_piece, "fsdp"), adapter_up_map, average_up_map)
    return (down_grad, up_grad, average_down_next, average_up_next, loss.reshape(()))


def solution(mesh):
    placed = (
        P(("dp", "fsdp"), None),
        P(("dp", "fsdp"), None),
        P(("dp", "fsdp"), None),
        P(("dp", "fsdp"), None),
        P(("dp", "fsdp")),
        P("fsdp", None),
        P("fsdp", None),
        P(),
        P("fsdp", None),
        P(),
    )
    return jax.shard_map(
        per_device,
        mesh=mesh,
        in_specs=placed,
        out_specs=(P("fsdp", None), P(), P("fsdp", None), P(), P()),
        check_vma=False,
    )
```

```python
import functools
import math

import jax
import jax.numpy as jnp
from jax import lax
from jax.experimental import pallas as pl
from jax.experimental.pallas import tpu as pltpu
from jax.sharding import PartitionSpec as P


HEADS = 16
KEY_VALUE_HEADS = 4
HEAD_DIM = 128
GROUP = HEADS // KEY_VALUE_HEADS
TOK = 256
MODEL = 4096
RANK = 64
KV_WIDTH = KEY_VALUE_HEADS * HEAD_DIM
WIDTH = KV_WIDTH + RANK
PADDED = KV_WIDTH + HEAD_DIM

adapter_scale = 2.0
average_decay = 0.9
learning_rate = 1.0
masked_score = -1e30

PIECE_ROWS = 40
SMALL = pltpu.CompilerParams(vmem_limit_bytes=4 * 2**20)


def nt(a, b):
    return lax.dot_general(a, b, (((1,), (1,)), ((), ())), preferred_element_type=jnp.float32)


def nn(a, b):
    return lax.dot_general(a, b, (((1,), (0,)), ((), ())), preferred_element_type=jnp.float32)


def probs_kernel(length_ref, q_ref, k_ref, p_ref, pt_ref):
    length = length_ref[0]
    keys = k_ref[...]
    row = lax.broadcasted_iota(jnp.int32, (TOK, TOK), 0)
    col = lax.broadcasted_iota(jnp.int32, (TOK, TOK), 1)
    allowed = (col <= row) & (col < length)
    for g in range(GROUP):
        scores = nt(q_ref[:, g * HEAD_DIM : (g + 1) * HEAD_DIM], keys) * (1.0 / math.sqrt(HEAD_DIM))
        scores = jnp.where(allowed, scores, masked_score)
        weights = jnp.exp(scores - jnp.max(scores, axis=-1, keepdims=True))
        probs = weights * (1.0 / jnp.sum(weights, axis=-1, keepdims=True))
        p_ref[0, g * TOK : (g + 1) * TOK, :] = probs.astype(jnp.bfloat16)
        pt_ref[0, :, g * TOK : (g + 1) * TOK] = jnp.transpose(probs).astype(jnp.bfloat16)


def attention_probs(lengths, queries, keys):
    shape = jax.ShapeDtypeStruct
    return pl.pallas_call(
        probs_kernel,
        grid=(KEY_VALUE_HEADS,),
        in_specs=[
            pl.BlockSpec(memory_space=pltpu.SMEM),
            pl.BlockSpec((TOK, GROUP * HEAD_DIM), lambda h: (0, h)),
            pl.BlockSpec((TOK, HEAD_DIM), lambda h: (0, h)),
        ],
        out_specs=[
            pl.BlockSpec((1, GROUP * TOK, TOK), lambda h: (h, 0, 0)),
            pl.BlockSpec((1, TOK, GROUP * TOK), lambda h: (h, 0, 0)),
        ],
        out_shape=[
            shape((KEY_VALUE_HEADS, GROUP * TOK, TOK), jnp.bfloat16),
            shape((KEY_VALUE_HEADS, TOK, GROUP * TOK), jnp.bfloat16),
        ],
        compiler_params=pltpu.CompilerParams(vmem_limit_bytes=16 * 2**20),
        cost_estimate=pl.CostEstimate(flops=2**31, bytes_accessed=6 * 2**20, transcendentals=2**20),
        name="probs",
    )(lengths, queries, keys)


def pack_kernel(value_ref, down_ref, out_ref):
    down = down_ref[...].astype(jnp.bfloat16)
    for d in range(out_ref.shape[0]):
        out_ref[d, :, :KV_WIDTH] = value_ref[...]
        out_ref[d, :, KV_WIDTH:] = down


def packed_shard(value_rows, down_rows, copies):
    return pl.pallas_call(
        pack_kernel,
        out_shape=jax.ShapeDtypeStruct((copies, RANK, WIDTH), jnp.bfloat16),
        compiler_params=SMALL,
        name="pack",
    )(value_rows, down_rows)


def split_kernel(facts_ref, hidden, keep, send):
    first = lax.broadcasted_iota(jnp.int32, (TOK, HEAD_DIM), 1) < RANK
    mine = facts_ref[1] == 0
    for x in range(4):
        for y in range(0, 8, 2):
            a = hidden[:, y * 512 + x * 128 : y * 512 + (x + 1) * 128].astype(jnp.float32)
            b = hidden[:, (y + 1) * 512 + x * 128 : (y + 1) * 512 + (x + 1) * 128].astype(jnp.float32)
            even = jnp.where(first, a, pltpu.roll(b, RANK, 1))
            odd = jnp.where(first, pltpu.roll(a, RANK, 1), b)
            to = pl.ds(x * 512 + y * 64, 128)
            keep[:, to] = jnp.where(mine, even, odd).astype(jnp.bfloat16)
            send[:, to] = jnp.where(mine, odd, even).astype(jnp.bfloat16)


def split_hidden(facts, hidden):
    vmem = pl.BlockSpec(memory_space=pltpu.VMEM)
    shape = jax.ShapeDtypeStruct((TOK, MODEL // 2), jnp.bfloat16)
    return pl.pallas_call(
        split_kernel,
        in_specs=[pl.BlockSpec(memory_space=pltpu.SMEM), vmem],
        out_specs=[vmem, vmem],
        out_shape=[shape, shape],
        compiler_params=pltpu.CompilerParams(vmem_limit_bytes=12 * 2**20),
        cost_estimate=pl.CostEstimate(flops=2**30, bytes_accessed=2**22, transcendentals=0),
        name="split",
    )(facts, hidden)


def partial_kernel(which, facts_ref, mine, theirs, *rest):
    *blocks, before, out = rest
    column = lax.rem(facts_ref[2] + (4 - which), 4) * 512
    half = facts_ref[3] * 256
    for i, tokens in enumerate((mine, theirs)):
        if len(blocks) == 1:
            part = nn(
                tokens[:, pl.ds(pl.multiple_of(column, 512), 512)], blocks[0][...].reshape(512, WIDTH)
            )
        else:
            part = nn(
                tokens[:, pl.ds(pl.multiple_of(column + half, 256), 256)], blocks[0][...].reshape(256, WIDTH)
            )
            rows = jnp.concatenate([blocks[1][...].reshape(128, WIDTH), blocks[2][...].reshape(128, WIDTH)], axis=0)
            part += nn(tokens[:, pl.ds(pl.multiple_of(column + (256 - half), 256), 256)], rows)
        out[i] = part if before is None else part + before[i]


def first_partial_kernel(which, facts_ref, mine, theirs, block, out):
    partial_kernel(which, facts_ref, mine, theirs, block, None, out)


def last_partial_kernel(which, facts_ref, mine, theirs, half, low, high, before, own, other):
    class Outs:
        def __setitem__(self, i, value):
            (own, other)[i][:, :WIDTH] = value

    partial_kernel(which, facts_ref, mine, theirs, half, low, high, before, Outs())
    for out in (own, other):
        out[:, WIDTH:] = jnp.zeros((TOK, PADDED - WIDTH), jnp.float32)


def partial_values(facts, mine, theirs, blocks, which, before=None):
    vmem = pl.BlockSpec(memory_space=pltpu.VMEM)
    given = tuple(blocks) + (() if before is None else (before,))
    last = len(blocks) > 1
    body = last_partial_kernel if last else first_partial_kernel if before is None else partial_kernel
    shape = jax.ShapeDtypeStruct((TOK, PADDED), jnp.float32)
    return pl.pallas_call(
        functools.partial(body, which),
        in_specs=[pl.BlockSpec(memory_space=pltpu.SMEM)] + [vmem] * (2 + len(given)),
        out_specs=[vmem, vmem] if last else vmem,
        out_shape=[shape, shape] if last else jax.ShapeDtypeStruct((2, TOK, WIDTH), jnp.float32),
        compiler_params=pltpu.CompilerParams(vmem_limit_bytes=12 * 2**20),
        cost_estimate=pl.CostEstimate(flops=2**29, bytes_accessed=2**21, transcendentals=0),
        name="partial",
    )(facts, mine, theirs, *given)


def grads_kernel(
    facts_ref, hidden, before, swapped, probs, probs_t, target, up_ref, out_ref, cot, value_grad,
):
    length = facts_ref[0]
    up = up_ref[...].astype(jnp.bfloat16)
    total = before[...] + swapped[...]
    latent = total[:, KV_WIDTH:WIDTH].astype(jnp.bfloat16)
    values = (total[:, :KV_WIDTH] + adapter_scale * nn(latent, up)).astype(jnp.bfloat16)

    live = lax.broadcasted_iota(jnp.int32, (TOK, HEAD_DIM), 0) < length
    squares = jnp.zeros((TOK, HEAD_DIM), jnp.float32)
    for k in range(KEY_VALUE_HEADS):
        output = nn(probs[k], values[:, k * HEAD_DIM : (k + 1) * HEAD_DIM])
        for g in range(GROUP):
            h = k * GROUP + g
            aim = target[:, h * HEAD_DIM : (h + 1) * HEAD_DIM].astype(jnp.float32)
            differ = jnp.where(live, output[g * TOK : (g + 1) * TOK, :] - aim, 0.0)
            squares = squares + differ * differ
            cot[g * TOK : (g + 1) * TOK, :] = differ.astype(jnp.bfloat16)
        value_grad[:, k * HEAD_DIM : (k + 1) * HEAD_DIM] = nn(probs_t[k], cot[...]).astype(jnp.bfloat16)

    grad = value_grad[...]
    latent_grad_t = nt(up, grad).astype(jnp.bfloat16)
    up_term = lax.dot_general(latent, grad, (((0,), (0,)), ((), ())), preferred_element_type=jnp.float32)

    lane = lax.broadcasted_iota(jnp.int32, (RANK // 2, HEAD_DIM), 1) < RANK
    for m in range(MODEL // 512):
        term = nn(latent_grad_t, hidden[:, m * 512 : (m + 1) * 512])
        for i in range(4):
            a = term[: RANK // 2, i * 128 : (i + 1) * 128]
            b = term[RANK // 2 :, i * 128 : (i + 1) * 128]
            even = jnp.where(lane, a, pltpu.roll(b, RANK, 1))
            odd = jnp.where(lane, pltpu.roll(a, RANK, 1), b)
            out_ref[m * 8 + 2 * i, :32, :] = even.astype(jnp.bfloat16)
            out_ref[m * 8 + 2 * i + 1, :32, :] = odd.astype(jnp.bfloat16)

    loss = jnp.sum(jnp.sum(squares, axis=0, keepdims=True), axis=1, keepdims=True)
    high = loss.astype(jnp.bfloat16).astype(jnp.float32)
    sub8 = lax.broadcasted_iota(jnp.int32, (8, HEAD_DIM), 0)
    lane8 = lax.broadcasted_iota(jnp.int32, (8, HEAD_DIM), 1)
    count = jnp.full((8, HEAD_DIM), length, jnp.int32).astype(jnp.float32)
    facts = jnp.where(lane8 == 0, high, jnp.where(lane8 == 1, loss - high, jnp.where(lane8 == 2, count, 0.0)))
    for q in range(8):
        for b in range(4):
            tile = up_term[8 * q : 8 * q + 8, b * 128 : (b + 1) * 128]
            out_ref[8 * q + b, 32:, :] = jnp.where(sub8 < 4, tile, facts).astype(jnp.bfloat16)
            out_ref[8 * q + 4 + b, 32:, :] = jnp.where(sub8 < 4, pltpu.roll(tile, 4, 0), facts).astype(jnp.bfloat16)


def gradient_pieces(facts, hidden, before, swapped, probs, probs_t, target, up_map):
    vmem = pl.BlockSpec(memory_space=pltpu.VMEM)
    return pl.pallas_call(
        grads_kernel,
        in_specs=[pl.BlockSpec(memory_space=pltpu.SMEM)] + [vmem] * 7,
        out_specs=vmem,
        out_shape=jax.ShapeDtypeStruct((MODEL // RANK, PIECE_ROWS, HEAD_DIM), jnp.bfloat16),
        scratch_shapes=[
            pltpu.VMEM((GROUP * TOK, HEAD_DIM), jnp.bfloat16),
            pltpu.VMEM((TOK, KV_WIDTH), jnp.bfloat16),
        ],
        compiler_params=pltpu.CompilerParams(vmem_limit_bytes=24 * 2**20),
        cost_estimate=pl.CostEstimate(flops=2**32, bytes_accessed=10 * 2**20, transcendentals=0),
        name="grads",
    )(facts, hidden, before, swapped, probs, probs_t, target, up_map)


def fold_kernel(pieces_ref, out_ref):
    total = jnp.sum(pieces_ref[...].astype(jnp.float32), axis=0)
    for d in range(out_ref.shape[0]):
        out_ref[d] = total


def fold(pieces, copies):
    return pl.pallas_call(
        fold_kernel,
        out_shape=jax.ShapeDtypeStruct((copies, PIECE_ROWS, HEAD_DIM), jnp.float32),
        compiler_params=SMALL,
        name="fold",
    )(pieces)


def owner_kernel(pieces_ref, down_ref, average_ref, grad_ref, next_ref, up_ref, loss_ref):
    total = jnp.sum(pieces_ref[...], axis=0)
    count = total[36:37, 2:3]
    loss_ref[...] = (total[36:37, 0:1] + total[36:37, 1:2]) / (2.0 * count)
    factor = adapter_scale / count
    rows = jnp.concatenate([total[:32, :RANK], total[:32, RANK:]], axis=0)
    grad = jnp.transpose(rows) * factor
    grad_ref[...] = grad
    next_ref[...] = average_decay * average_ref[...] + (1.0 - average_decay) * (down_ref[...] - learning_rate * grad)
    piece = total[32:36, :] * factor
    for d in range(up_ref.shape[0]):
        up_ref[d] = piece


def owner_update(pieces, down_map, average_down_map, copies):
    shape = jax.ShapeDtypeStruct
    return pl.pallas_call(
        owner_kernel,
        out_shape=[
            shape((RANK, RANK), jnp.float32),
            shape((RANK, RANK), jnp.float32),
            shape((copies, 4, HEAD_DIM), jnp.float32),
            shape((1, 1), jnp.float32),
        ],
        compiler_params=SMALL,
        name="owner",
    )(pieces, down_map, average_down_map)


def second_kernel(pieces_ref, up_ref, average_ref, grad_ref, next_ref):
    for j in range(MODEL // RANK):
        q, b = divmod(j, 4)
        grad_ref[4 * q : 4 * q + 4, b * 128 : (b + 1) * 128] = pieces_ref[j]
    next_ref[...] = average_decay * average_ref[...] + (1.0 - average_decay) * (
        up_ref[...] - learning_rate * grad_ref[...]
    )


def second_update(pieces, up_map, average_up_map):
    shape = jax.ShapeDtypeStruct((RANK, KV_WIDTH), jnp.float32)
    return pl.pallas_call(second_kernel, out_shape=[shape, shape], compiler_params=SMALL, name="second")(
        pieces, up_map, average_up_map
    )


def exchange(pieces, axis):
    return lax.all_to_all(pieces, axis, 0, 0, tiled=True)


def along_y(owners):
    return [list(range(k, owners, 8)) for k in range(8)]


def along_x(block, owners, shift):
    moved = [(i, i // 8 * 8 + (i + 2 * shift) % 8) for i in range(owners)]
    return lax.ppermute(block, "fsdp", moved)


def from_other_core(block, owners):
    return lax.ppermute(block, "fsdp", [(i, i ^ 1) for i in range(owners)])


def per_device(
    hidden,
    queries,
    keys,
    target,
    lengths,
    value_weight_frozen,
    adapter_down_map,
    adapter_up_map,
    average_down_map,
    average_up_map,
):
    owners, replicas = lax.axis_size("fsdp"), lax.axis_size("dp")
    place = lax.axis_index("fsdp").astype(jnp.int32)
    parity = lax.axis_index("dp").astype(jnp.int32) & 1
    facts = jnp.stack([lengths[0], place & 1, (place >> 1) & 3, parity])
    shards = packed_shard(value_weight_frozen, adapter_down_map, owners // 8)
    own = lax.all_to_all(shards, "fsdp", 0, 0, tiled=True, axis_index_groups=along_y(owners))
    mine, send = split_hidden(facts, hidden)
    theirs = from_other_core(send, owners)
    probs, probs_t = attention_probs(lengths, queries, keys)
    half = along_x(lax.dynamic_slice_in_dim(own, parity * 4, 4, axis=0), owners, 2)
    near = along_x(own, owners, 1)
    far = along_x(own, owners, 3)
    low = lax.ppermute(half[:2], "dp", [(i, (i + 1) % replicas) for i in range(replicas)])
    high = lax.ppermute(half[2:], "dp", [(i, (i - 1) % replicas) for i in range(replicas)])
    total = None
    for shift, block in ((0, own), (1, near), (3, far)):
        total = partial_values(facts, mine, theirs, (block,), shift, total)
    total, other = partial_values(facts, mine, theirs, (half, low, high), 2, total)
    swapped = from_other_core(other, owners)
    pieces = gradient_pieces(facts, hidden, total, swapped, probs, probs_t, target, adapter_up_map)
    summed = fold(exchange(pieces, "fsdp"), replicas)
    down_grad, average_down_next, up_piece, loss = owner_update(
        exchange(summed, "dp"), adapter_down_map, average_down_map, owners
    )
    up_grad, average_up_next = second_update(exchange(up_piece, "fsdp"), adapter_up_map, average_up_map)
    return (down_grad, up_grad, average_down_next, average_up_next, loss.reshape(()))


def solution(mesh):
    placed = (
        P(("dp", "fsdp"), None),
        P(("dp", "fsdp"), None),
        P(("dp", "fsdp"), None),
        P(("dp", "fsdp"), None),
        P(("dp", "fsdp")),
        P("fsdp", None),
        P("fsdp", None),
        P(),
        P("fsdp", None),
        P(),
    )
    return jax.shard_map(
        per_device,
        mesh=mesh,
        in_specs=placed,
        out_specs=(P("fsdp", None), P(), P("fsdp", None), P(), P()),
        check_vma=False,
    )
```

```python
import functools
import math

import jax
import jax.numpy as jnp
from jax import lax
from jax.experimental import pallas as pl
from jax.experimental.pallas import tpu as pltpu
from jax.sharding import PartitionSpec as P


HEADS = 16
KEY_VALUE_HEADS = 4
HEAD_DIM = 128
GROUP = HEADS // KEY_VALUE_HEADS
TOK = 256
MODEL = 4096
RANK = 64
KV_WIDTH = KEY_VALUE_HEADS * HEAD_DIM
WIDTH = KV_WIDTH + RANK
PADDED = KV_WIDTH + HEAD_DIM

adapter_scale = 2.0
average_decay = 0.9
learning_rate = 1.0
masked_score = -1e30

PIECE_ROWS = 40
SMALL = pltpu.CompilerParams(vmem_limit_bytes=4 * 2**20)


def nt(a, b):
    return lax.dot_general(a, b, (((1,), (1,)), ((), ())), preferred_element_type=jnp.float32)


def nn(a, b):
    return lax.dot_general(a, b, (((1,), (0,)), ((), ())), preferred_element_type=jnp.float32)


def probs_kernel(length_ref, q_ref, k_ref, p_ref, pt_ref):
    length = length_ref[0]
    keys = k_ref[...]
    row = lax.broadcasted_iota(jnp.int32, (TOK, TOK), 0)
    col = lax.broadcasted_iota(jnp.int32, (TOK, TOK), 1)
    allowed = (col <= row) & (col < length)
    for g in range(GROUP):
        scores = nt(q_ref[:, g * HEAD_DIM : (g + 1) * HEAD_DIM], keys) * (1.0 / math.sqrt(HEAD_DIM))
        scores = jnp.where(allowed, scores, masked_score)
        weights = jnp.exp(scores - jnp.max(scores, axis=-1, keepdims=True))
        probs = weights * (1.0 / jnp.sum(weights, axis=-1, keepdims=True))
        p_ref[0, g * TOK : (g + 1) * TOK, :] = probs.astype(jnp.bfloat16)
        pt_ref[0, :, g * TOK : (g + 1) * TOK] = jnp.transpose(probs).astype(jnp.bfloat16)


def attention_probs(lengths, queries, keys):
    shape = jax.ShapeDtypeStruct
    return pl.pallas_call(
        probs_kernel,
        grid=(KEY_VALUE_HEADS,),
        in_specs=[
            pl.BlockSpec(memory_space=pltpu.SMEM),
            pl.BlockSpec((TOK, GROUP * HEAD_DIM), lambda h: (0, h)),
            pl.BlockSpec((TOK, HEAD_DIM), lambda h: (0, h)),
        ],
        out_specs=[
            pl.BlockSpec((1, GROUP * TOK, TOK), lambda h: (h, 0, 0)),
            pl.BlockSpec((1, TOK, GROUP * TOK), lambda h: (h, 0, 0)),
        ],
        out_shape=[
            shape((KEY_VALUE_HEADS, GROUP * TOK, TOK), jnp.bfloat16),
            shape((KEY_VALUE_HEADS, TOK, GROUP * TOK), jnp.bfloat16),
        ],
        compiler_params=pltpu.CompilerParams(vmem_limit_bytes=16 * 2**20),
        cost_estimate=pl.CostEstimate(flops=2**31, bytes_accessed=6 * 2**20, transcendentals=2**20),
        name="probs",
    )(lengths, queries, keys)


def pack_kernel(value_ref, down_ref, out_ref):
    down = down_ref[...].astype(jnp.bfloat16)
    for d in range(out_ref.shape[0]):
        out_ref[d, :, :KV_WIDTH] = value_ref[...]
        out_ref[d, :, KV_WIDTH:] = down


def packed_shard(value_rows, down_rows, copies):
    return pl.pallas_call(
        pack_kernel,
        out_shape=jax.ShapeDtypeStruct((copies, RANK, WIDTH), jnp.bfloat16),
        compiler_params=SMALL,
        name="pack",
    )(value_rows, down_rows)


def split_kernel(facts_ref, hidden, keep, send):
    first = lax.broadcasted_iota(jnp.int32, (TOK, HEAD_DIM), 1) < RANK
    mine = facts_ref[1] == 0
    for x in range(4):
        for y in range(0, 8, 2):
            a = hidden[:, y * 512 + x * 128 : y * 512 + (x + 1) * 128].astype(jnp.float32)
            b = hidden[:, (y + 1) * 512 + x * 128 : (y + 1) * 512 + (x + 1) * 128].astype(jnp.float32)
            even = jnp.where(first, a, pltpu.roll(b, RANK, 1))
            odd = jnp.where(first, pltpu.roll(a, RANK, 1), b)
            to = pl.ds(x * 512 + y * 64, 128)
            keep[:, to] = jnp.where(mine, even, odd).astype(jnp.bfloat16)
            send[:, to] = jnp.where(mine, odd, even).astype(jnp.bfloat16)


def split_hidden(facts, hidden):
    vmem = pl.BlockSpec(memory_space=pltpu.VMEM)
    shape = jax.ShapeDtypeStruct((TOK, MODEL // 2), jnp.bfloat16)
    return pl.pallas_call(
        split_kernel,
        in_specs=[pl.BlockSpec(memory_space=pltpu.SMEM), vmem],
        out_specs=[vmem, vmem],
        out_shape=[shape, shape],
        compiler_params=pltpu.CompilerParams(vmem_limit_bytes=12 * 2**20),
        cost_estimate=pl.CostEstimate(flops=2**30, bytes_accessed=2**22, transcendentals=0),
        name="split",
    )(facts, hidden)


def partial_kernel(which, facts_ref, mine, theirs, *rest):
    *blocks, before, out = rest
    column = lax.rem(facts_ref[2] + (4 - which), 4) * 512
    for i, tokens in enumerate((mine, theirs)):
        if len(blocks) == 1:
            part = nn(tokens[:, pl.ds(pl.multiple_of(column, 512), 512)], blocks[0][...].reshape(512, WIDTH))
        else:
            part = None
            for j in (0, 2):
                left, right = [], []
                for k in (j, j + 1):
                    quarter = facts_ref[3] ^ k
                    left.append(tokens[:, pl.ds(pl.multiple_of(column + quarter * 128, 128), 128)])
                    right.append(blocks[k][...].reshape(128, WIDTH))
                more = nn(jnp.concatenate(left, axis=1), jnp.concatenate(right, axis=0))
                part = more if part is None else part + more
        out[i] = part if before is None else part + before[i]


def first_partial_kernel(which, facts_ref, mine, theirs, block, out):
    partial_kernel(which, facts_ref, mine, theirs, block, None, out)


def last_partial_kernel(which, facts_ref, mine, theirs, block, before, own, other):
    class Outs:
        def __setitem__(self, i, value):
            (own, other)[i][:, :WIDTH] = value

    partial_kernel(which, facts_ref, mine, theirs, block, before, Outs())
    for out in (own, other):
        out[:, WIDTH:] = jnp.zeros((TOK, PADDED - WIDTH), jnp.float32)


def partial_values(facts, mine, theirs, blocks, which, before=None, last=False):
    vmem = pl.BlockSpec(memory_space=pltpu.VMEM)
    given = tuple(blocks) + (() if before is None else (before,))
    body = last_partial_kernel if last else first_partial_kernel if before is None else partial_kernel
    shape = jax.ShapeDtypeStruct((TOK, PADDED), jnp.float32)
    return pl.pallas_call(
        functools.partial(body, which),
        in_specs=[pl.BlockSpec(memory_space=pltpu.SMEM)] + [vmem] * (2 + len(given)),
        out_specs=[vmem, vmem] if last else vmem,
        out_shape=[shape, shape] if last else jax.ShapeDtypeStruct((2, TOK, WIDTH), jnp.float32),
        compiler_params=pltpu.CompilerParams(vmem_limit_bytes=12 * 2**20),
        cost_estimate=pl.CostEstimate(flops=2**29, bytes_accessed=2**21, transcendentals=0),
        name="partial",
    )(facts, mine, theirs, *given)


def grads_kernel(
    facts_ref, hidden, before, swapped, probs, probs_t, target, up_ref, out_ref, cot, value_grad,
):
    length = facts_ref[0]
    up = up_ref[...].astype(jnp.bfloat16)
    total = before[...] + swapped[...]
    latent = total[:, KV_WIDTH:WIDTH].astype(jnp.bfloat16)
    values = (total[:, :KV_WIDTH] + adapter_scale * nn(latent, up)).astype(jnp.bfloat16)

    live = lax.broadcasted_iota(jnp.int32, (TOK, HEAD_DIM), 0) < length
    squares = jnp.zeros((TOK, HEAD_DIM), jnp.float32)
    for k in range(KEY_VALUE_HEADS):
        output = nn(probs[k], values[:, k * HEAD_DIM : (k + 1) * HEAD_DIM])
        for g in range(GROUP):
            h = k * GROUP + g
            aim = target[:, h * HEAD_DIM : (h + 1) * HEAD_DIM].astype(jnp.float32)
            differ = jnp.where(live, output[g * TOK : (g + 1) * TOK, :] - aim, 0.0)
            squares = squares + differ * differ
            cot[g * TOK : (g + 1) * TOK, :] = differ.astype(jnp.bfloat16)
        value_grad[:, k * HEAD_DIM : (k + 1) * HEAD_DIM] = nn(probs_t[k], cot[...]).astype(jnp.bfloat16)

    grad = value_grad[...]
    latent_grad_t = nt(up, grad).astype(jnp.bfloat16)
    up_term = lax.dot_general(latent, grad, (((0,), (0,)), ((), ())), preferred_element_type=jnp.float32)

    lane = lax.broadcasted_iota(jnp.int32, (RANK // 2, HEAD_DIM), 1) < RANK
    for m in range(MODEL // 512):
        term = nn(latent_grad_t, hidden[:, m * 512 : (m + 1) * 512])
        for i in range(4):
            a = term[: RANK // 2, i * 128 : (i + 1) * 128]
            b = term[RANK // 2 :, i * 128 : (i + 1) * 128]
            even = jnp.where(lane, a, pltpu.roll(b, RANK, 1))
            odd = jnp.where(lane, pltpu.roll(a, RANK, 1), b)
            out_ref[m * 8 + 2 * i, :32, :] = even.astype(jnp.bfloat16)
            out_ref[m * 8 + 2 * i + 1, :32, :] = odd.astype(jnp.bfloat16)

    loss = jnp.sum(jnp.sum(squares, axis=0, keepdims=True), axis=1, keepdims=True)
    high = loss.astype(jnp.bfloat16).astype(jnp.float32)
    sub8 = lax.broadcasted_iota(jnp.int32, (8, HEAD_DIM), 0)
    lane8 = lax.broadcasted_iota(jnp.int32, (8, HEAD_DIM), 1)
    count = jnp.full((8, HEAD_DIM), length, jnp.int32).astype(jnp.float32)
    facts = jnp.where(lane8 == 0, high, jnp.where(lane8 == 1, loss - high, jnp.where(lane8 == 2, count, 0.0)))
    for q in range(8):
        for b in range(4):
            tile = up_term[8 * q : 8 * q + 8, b * 128 : (b + 1) * 128]
            out_ref[8 * q + b, 32:, :] = jnp.where(sub8 < 4, tile, facts).astype(jnp.bfloat16)
            out_ref[8 * q + 4 + b, 32:, :] = jnp.where(sub8 < 4, pltpu.roll(tile, 4, 0), facts).astype(jnp.bfloat16)


def gradient_pieces(facts, hidden, before, swapped, probs, probs_t, target, up_map):
    vmem = pl.BlockSpec(memory_space=pltpu.VMEM)
    return pl.pallas_call(
        grads_kernel,
        in_specs=[pl.BlockSpec(memory_space=pltpu.SMEM)] + [vmem] * 7,
        out_specs=vmem,
        out_shape=jax.ShapeDtypeStruct((MODEL // RANK, PIECE_ROWS, HEAD_DIM), jnp.bfloat16),
        scratch_shapes=[
            pltpu.VMEM((GROUP * TOK, HEAD_DIM), jnp.bfloat16),
            pltpu.VMEM((TOK, KV_WIDTH), jnp.bfloat16),
        ],
        compiler_params=pltpu.CompilerParams(vmem_limit_bytes=24 * 2**20),
        cost_estimate=pl.CostEstimate(flops=2**32, bytes_accessed=10 * 2**20, transcendentals=0),
        name="grads",
    )(facts, hidden, before, swapped, probs, probs_t, target, up_map)


def fold_kernel(pieces_ref, out_ref):
    total = jnp.sum(pieces_ref[...].astype(jnp.float32), axis=0)
    for d in range(out_ref.shape[0]):
        out_ref[d] = total


def fold(pieces, copies):
    return pl.pallas_call(
        fold_kernel,
        out_shape=jax.ShapeDtypeStruct((copies, PIECE_ROWS, HEAD_DIM), jnp.float32),
        compiler_params=SMALL,
        name="fold",
    )(pieces)


def owner_kernel(pieces_ref, down_ref, average_ref, grad_ref, next_ref, up_ref, loss_ref):
    total = jnp.sum(pieces_ref[...], axis=0)
    count = total[36:37, 2:3]
    loss_ref[...] = (total[36:37, 0:1] + total[36:37, 1:2]) / (2.0 * count)
    factor = adapter_scale / count
    rows = jnp.concatenate([total[:32, :RANK], total[:32, RANK:]], axis=0)
    grad = jnp.transpose(rows) * factor
    grad_ref[...] = grad
    next_ref[...] = average_decay * average_ref[...] + (1.0 - average_decay) * (down_ref[...] - learning_rate * grad)
    piece = total[32:36, :] * factor
    for d in range(up_ref.shape[0]):
        up_ref[d] = piece


def owner_update(pieces, down_map, average_down_map, copies):
    shape = jax.ShapeDtypeStruct
    return pl.pallas_call(
        owner_kernel,
        out_shape=[
            shape((RANK, RANK), jnp.float32),
            shape((RANK, RANK), jnp.float32),
            shape((copies, 4, HEAD_DIM), jnp.float32),
            shape((1, 1), jnp.float32),
        ],
        compiler_params=SMALL,
        name="owner",
    )(pieces, down_map, average_down_map)


def second_kernel(pieces_ref, up_ref, average_ref, grad_ref, next_ref):
    for j in range(MODEL // RANK):
        q, b = divmod(j, 4)
        grad_ref[4 * q : 4 * q + 4, b * 128 : (b + 1) * 128] = pieces_ref[j]
    next_ref[...] = average_decay * average_ref[...] + (1.0 - average_decay) * (
        up_ref[...] - learning_rate * grad_ref[...]
    )


def second_update(pieces, up_map, average_up_map):
    shape = jax.ShapeDtypeStruct((RANK, KV_WIDTH), jnp.float32)
    return pl.pallas_call(second_kernel, out_shape=[shape, shape], compiler_params=SMALL, name="second")(
        pieces, up_map, average_up_map
    )


def exchange(pieces, axis):
    return lax.all_to_all(pieces, axis, 0, 0, tiled=True)


def along_y(owners):
    return [list(range(k, owners, 8)) for k in range(8)]


def along_x(block, owners, shift):
    moved = [(i, i // 8 * 8 + (i + 2 * shift) % 8) for i in range(owners)]
    return lax.ppermute(block, "fsdp", moved)


def from_neighbour(part, owners, replicas, y, z):
    moved = [
        ((d + z) % replicas * owners + (i + 8 * y) % owners, d * owners + i)
        for d in range(replicas)
        for i in range(owners)
    ]
    return lax.ppermute(part, ("dp", "fsdp"), moved)


def from_other_core(block, owners):
    return lax.ppermute(block, "fsdp", [(i, i ^ 1) for i in range(owners)])


def per_device(
    hidden,
    queries,
    keys,
    target,
    lengths,
    value_weight_frozen,
    adapter_down_map,
    adapter_up_map,
    average_down_map,
    average_up_map,
):
    owners, replicas = lax.axis_size("fsdp"), lax.axis_size("dp")
    place = lax.axis_index("fsdp").astype(jnp.int32)
    plane = lax.axis_index("dp").astype(jnp.int32)
    quarter = (plane & 1) * 2 + ((place >> 3) & 1)
    facts = jnp.stack([lengths[0], place & 1, (place >> 1) & 3, quarter])
    shards = packed_shard(value_weight_frozen, adapter_down_map, owners // 8)
    own = lax.all_to_all(shards, "fsdp", 0, 0, tiled=True, axis_index_groups=along_y(owners))
    mine, send = split_hidden(facts, hidden)
    theirs = from_other_core(send, owners)
    probs, probs_t = attention_probs(lengths, queries, keys)
    part = along_x(lax.dynamic_slice_in_dim(own, quarter * 2, 2, axis=0), owners, 2)
    near = along_x(own, owners, 1)
    far = along_x(own, owners, 3)
    beside = from_neighbour(part, owners, replicas, 1, 0)
    behind = from_neighbour(part, owners, replicas, 0, 1)
    corner = from_neighbour(part, owners, replicas, 1, 1)
    total = None
    for shift, given in ((0, (own,)), (3, (far,)), (2, (part, beside, behind, corner))):
        total = partial_values(facts, mine, theirs, given, shift, total)
    total, other = partial_values(facts, mine, theirs, (near,), 1, total, last=True)
    swapped = from_other_core(other, owners)
    pieces = gradient_pieces(facts, hidden, total, swapped, probs, probs_t, target, adapter_up_map)
    summed = fold(exchange(pieces, "fsdp"), replicas)
    down_grad, average_down_next, up_piece, loss = owner_update(
        exchange(summed, "dp"), adapter_down_map, average_down_map, owners
    )
    up_grad, average_up_next = second_update(exchange(up_piece, "fsdp"), adapter_up_map, average_up_map)
    return (down_grad, up_grad, average_down_next, average_up_next, loss.reshape(()))


def solution(mesh):
    placed = (
        P(("dp", "fsdp"), None),
        P(("dp", "fsdp"), None),
        P(("dp", "fsdp"), None),
        P(("dp", "fsdp"), None),
        P(("dp", "fsdp")),
        P("fsdp", None),
        P("fsdp", None),
        P(),
        P("fsdp", None),
        P(),
    )
    return jax.shard_map(
        per_device,
        mesh=mesh,
        in_specs=placed,
        out_specs=(P("fsdp", None), P(), P("fsdp", None), P(), P()),
        check_vma=False,
    )
```

```python
import functools
import math

import jax
import jax.numpy as jnp
from jax import lax
from jax.experimental import pallas as pl
from jax.experimental.pallas import tpu as pltpu
from jax.sharding import PartitionSpec as P


HEADS = 16
KEY_VALUE_HEADS = 4
HEAD_DIM = 128
GROUP = HEADS // KEY_VALUE_HEADS
TOK = 256
MODEL = 4096
RANK = 64
KV_WIDTH = KEY_VALUE_HEADS * HEAD_DIM
WIDTH = KV_WIDTH + RANK
PADDED = KV_WIDTH + HEAD_DIM

adapter_scale = 2.0
average_decay = 0.9
learning_rate = 1.0
masked_score = -1e30

PIECE_ROWS = 40
SMALL = pltpu.CompilerParams(vmem_limit_bytes=4 * 2**20)


def nt(a, b):
    return lax.dot_general(a, b, (((1,), (1,)), ((), ())), preferred_element_type=jnp.float32)


def nn(a, b):
    return lax.dot_general(a, b, (((1,), (0,)), ((), ())), preferred_element_type=jnp.float32)


def probs_kernel(length_ref, q_ref, k_ref, p_ref, pt_ref):
    length = length_ref[0]
    keys = k_ref[...]
    row = lax.broadcasted_iota(jnp.int32, (TOK, TOK), 0)
    col = lax.broadcasted_iota(jnp.int32, (TOK, TOK), 1)
    allowed = (col <= row) & (col < length)
    for g in range(GROUP):
        scores = nt(q_ref[:, g * HEAD_DIM : (g + 1) * HEAD_DIM], keys) * (1.0 / math.sqrt(HEAD_DIM))
        scores = jnp.where(allowed, scores, masked_score)
        weights = jnp.exp(scores - jnp.max(scores, axis=-1, keepdims=True))
        probs = weights * (1.0 / jnp.sum(weights, axis=-1, keepdims=True))
        p_ref[0, g * TOK : (g + 1) * TOK, :] = probs.astype(jnp.bfloat16)
        pt_ref[0, :, g * TOK : (g + 1) * TOK] = jnp.transpose(probs).astype(jnp.bfloat16)


def attention_probs(lengths, queries, keys):
    shape = jax.ShapeDtypeStruct
    return pl.pallas_call(
        probs_kernel,
        grid=(KEY_VALUE_HEADS,),
        in_specs=[
            pl.BlockSpec(memory_space=pltpu.SMEM),
            pl.BlockSpec((TOK, GROUP * HEAD_DIM), lambda h: (0, h)),
            pl.BlockSpec((TOK, HEAD_DIM), lambda h: (0, h)),
        ],
        out_specs=[
            pl.BlockSpec((1, GROUP * TOK, TOK), lambda h: (h, 0, 0)),
            pl.BlockSpec((1, TOK, GROUP * TOK), lambda h: (h, 0, 0)),
        ],
        out_shape=[
            shape((KEY_VALUE_HEADS, GROUP * TOK, TOK), jnp.bfloat16),
            shape((KEY_VALUE_HEADS, TOK, GROUP * TOK), jnp.bfloat16),
        ],
        compiler_params=pltpu.CompilerParams(vmem_limit_bytes=60 * 2**20),
        cost_estimate=pl.CostEstimate(flops=2**31, bytes_accessed=6 * 2**20, transcendentals=2**20),
        name="probs",
    )(lengths, queries, keys)


def pack_kernel(value_ref, down_ref, out_ref):
    down = down_ref[...].astype(jnp.bfloat16)
    for d in range(out_ref.shape[0]):
        out_ref[d, :, :KV_WIDTH] = value_ref[...]
        out_ref[d, :, KV_WIDTH:] = down


def packed_shard(value_rows, down_rows, copies):
    return pl.pallas_call(
        pack_kernel,
        out_shape=jax.ShapeDtypeStruct((copies, RANK, WIDTH), jnp.bfloat16),
        compiler_params=SMALL,
        name="pack",
    )(value_rows, down_rows)


def split_kernel(facts_ref, hidden, keep, send):
    first = lax.broadcasted_iota(jnp.int32, (TOK, HEAD_DIM), 1) < RANK
    mine = facts_ref[1] == 0
    for x in range(4):
        for y in range(0, 8, 2):
            a = hidden[:, y * 512 + x * 128 : y * 512 + (x + 1) * 128].astype(jnp.float32)
            b = hidden[:, (y + 1) * 512 + x * 128 : (y + 1) * 512 + (x + 1) * 128].astype(jnp.float32)
            even = jnp.where(first, a, pltpu.roll(b, RANK, 1))
            odd = jnp.where(first, pltpu.roll(a, RANK, 1), b)
            to = pl.ds(x * 512 + y * 64, 128)
            keep[:, to] = jnp.where(mine, even, odd).astype(jnp.bfloat16)
            send[:, to] = jnp.where(mine, odd, even).astype(jnp.bfloat16)


def split_hidden(facts, hidden):
    vmem = pl.BlockSpec(memory_space=pltpu.VMEM)
    shape = jax.ShapeDtypeStruct((TOK, MODEL // 2), jnp.bfloat16)
    return pl.pallas_call(
        split_kernel,
        in_specs=[pl.BlockSpec(memory_space=pltpu.SMEM), vmem],
        out_specs=[vmem, vmem],
        out_shape=[shape, shape],
        compiler_params=pltpu.CompilerParams(vmem_limit_bytes=12 * 2**20),
        cost_estimate=pl.CostEstimate(flops=2**30, bytes_accessed=2**22, transcendentals=0),
        name="split",
    )(facts, hidden)


def partial_kernel(which, facts_ref, mine, theirs, *rest):
    *blocks, before, out = rest
    column = lax.rem(facts_ref[2] + (4 - which), 4) * 512
    for i, tokens in enumerate((mine, theirs)):
        if len(blocks) == 1:
            part = nn(tokens[:, pl.ds(pl.multiple_of(column, 512), 512)], blocks[0][...].reshape(512, WIDTH))
        else:
            part = None
            for j in (0, 2):
                left, right = [], []
                for k in (j, j + 1):
                    quarter = facts_ref[3] ^ k
                    left.append(tokens[:, pl.ds(pl.multiple_of(column + quarter * 128, 128), 128)])
                    right.append(blocks[k][...].reshape(128, WIDTH))
                more = nn(jnp.concatenate(left, axis=1), jnp.concatenate(right, axis=0))
                part = more if part is None else part + more
        out[i] = part if before is None else part + before[i]


def first_partial_kernel(which, facts_ref, mine, theirs, block, out):
    partial_kernel(which, facts_ref, mine, theirs, block, None, out)


def last_partial_kernel(which, facts_ref, mine, theirs, block, before, own, other):
    class Outs:
        def __setitem__(self, i, value):
            (own, other)[i][:, :WIDTH] = value

    partial_kernel(which, facts_ref, mine, theirs, block, before, Outs())
    for out in (own, other):
        out[:, WIDTH:] = jnp.zeros((TOK, PADDED - WIDTH), jnp.float32)


def partial_values(facts, mine, theirs, blocks, which, before=None, last=False):
    vmem = pl.BlockSpec(memory_space=pltpu.VMEM)
    given = tuple(blocks) + (() if before is None else (before,))
    body = last_partial_kernel if last else first_partial_kernel if before is None else partial_kernel
    shape = jax.ShapeDtypeStruct((TOK, PADDED), jnp.float32)
    return pl.pallas_call(
        functools.partial(body, which),
        in_specs=[pl.BlockSpec(memory_space=pltpu.SMEM)] + [vmem] * (2 + len(given)),
        out_specs=[vmem, vmem] if last else vmem,
        out_shape=[shape, shape] if last else jax.ShapeDtypeStruct((2, TOK, WIDTH), jnp.float32),
        compiler_params=pltpu.CompilerParams(vmem_limit_bytes=12 * 2**20),
        cost_estimate=pl.CostEstimate(flops=2**29, bytes_accessed=2**21, transcendentals=0),
        name="partial",
    )(facts, mine, theirs, *given)


def store_pieces(out_ref, latent_grad_t, hidden, up_term, facts, core):
    lane = lax.broadcasted_iota(jnp.int32, (RANK // 2, HEAD_DIM), 1) < RANK
    for x in range(4):
        term = nn(latent_grad_t, hidden[:, x * 512 : (x + 1) * 512])
        for i in range(4):
            a = term[: RANK // 2, i * 128 : (i + 1) * 128]
            b = term[RANK // 2 :, i * 128 : (i + 1) * 128]
            out_ref[8 * i + x, :32, :] = jnp.where(lane, a, pltpu.roll(b, RANK, 1))
            out_ref[8 * i + 4 + x, :32, :] = jnp.where(lane, pltpu.roll(a, RANK, 1), b)
    sub = lax.broadcasted_iota(jnp.int32, (8, HEAD_DIM), 0)
    for q in range(8):
        for b in range(4):
            tile = up_term[8 * q : 8 * q + 8, b * 128 : (b + 1) * 128]
            rows = jnp.where(core == 0, tile, pltpu.roll(tile, 4, 0))
            out_ref[4 * q + b, 32:, :] = jnp.where(sub < 4, rows, facts)


def grads_kernel(
    facts_ref, hidden, before, swapped, probs, probs_t, target, up_ref,
    out_ref, latent_grad_ref, up_term_ref, sums_ref, cot, value_grad,
):
    length = facts_ref[0]
    up = up_ref[...].astype(jnp.bfloat16)
    total = before[...] + swapped[...]
    latent = total[:, KV_WIDTH:WIDTH].astype(jnp.bfloat16)
    values = (total[:, :KV_WIDTH] + adapter_scale * nn(latent, up)).astype(jnp.bfloat16)

    live = lax.broadcasted_iota(jnp.int32, (TOK, HEAD_DIM), 0) < length
    squares = jnp.zeros((TOK, HEAD_DIM), jnp.float32)
    for k in range(KEY_VALUE_HEADS):
        output = nn(probs[k], values[:, k * HEAD_DIM : (k + 1) * HEAD_DIM])
        for g in range(GROUP):
            h = k * GROUP + g
            aim = target[:, h * HEAD_DIM : (h + 1) * HEAD_DIM].astype(jnp.float32)
            differ = jnp.where(live, output[g * TOK : (g + 1) * TOK, :] - aim, 0.0)
            squares = squares + differ * differ
            cot[g * TOK : (g + 1) * TOK, :] = differ.astype(jnp.bfloat16)
        value_grad[:, k * HEAD_DIM : (k + 1) * HEAD_DIM] = nn(probs_t[k], cot[...]).astype(jnp.bfloat16)

    grad = value_grad[...]
    latent_grad_t = nt(up, grad).astype(jnp.bfloat16)
    up_term = lax.dot_general(latent, grad, (((0,), (0,)), ((), ())), preferred_element_type=jnp.float32)

    loss = jnp.sum(jnp.sum(squares, axis=0, keepdims=True), axis=1, keepdims=True)
    lane = lax.broadcasted_iota(jnp.int32, (8, HEAD_DIM), 1)
    row = lax.broadcasted_iota(jnp.int32, (8, HEAD_DIM), 0)
    count = jnp.full((8, HEAD_DIM), length, jnp.int32).astype(jnp.float32)
    sums = jnp.where(lane == 0, loss, jnp.where(lane == 1, count, 0.0))
    sums = jnp.where(row == 4, sums, 0.0)
    latent_grad_ref[...] = latent_grad_t
    up_term_ref[...] = up_term
    sums_ref[...] = sums
    store_pieces(out_ref, latent_grad_t, hidden, up_term, sums, 1 - facts_ref[1])


PIECES = jax.ShapeDtypeStruct((MODEL // RANK // 2, PIECE_ROWS, HEAD_DIM), jnp.float32)


def gradients(facts, hidden, before, swapped, probs, probs_t, target, up_map):
    vmem = pl.BlockSpec(memory_space=pltpu.VMEM)
    shape = jax.ShapeDtypeStruct
    return pl.pallas_call(
        grads_kernel,
        in_specs=[pl.BlockSpec(memory_space=pltpu.SMEM)] + [vmem] * 7,
        out_specs=[vmem] * 4,
        out_shape=[
            PIECES,
            shape((RANK, TOK), jnp.bfloat16),
            shape((RANK, KV_WIDTH), jnp.float32),
            shape((8, HEAD_DIM), jnp.float32),
        ],
        scratch_shapes=[
            pltpu.VMEM((GROUP * TOK, HEAD_DIM), jnp.bfloat16),
            pltpu.VMEM((TOK, KV_WIDTH), jnp.bfloat16),
        ],
        compiler_params=pltpu.CompilerParams(vmem_limit_bytes=24 * 2**20),
        cost_estimate=pl.CostEstimate(flops=2**32, bytes_accessed=10 * 2**20, transcendentals=0),
        name="grads",
    )(facts, hidden, before, swapped, probs, probs_t, target, up_map)


def keep_kernel(facts_ref, hidden, latent_grad_ref, up_term_ref, sums_ref, out_ref):
    store_pieces(out_ref, latent_grad_ref[...], hidden, up_term_ref[...], sums_ref[...], facts_ref[1])


def kept_pieces(facts, hidden, latent_grad_t, up_term, sums):
    vmem = pl.BlockSpec(memory_space=pltpu.VMEM)
    return pl.pallas_call(
        keep_kernel,
        in_specs=[pl.BlockSpec(memory_space=pltpu.SMEM)] + [vmem] * 4,
        out_specs=vmem,
        out_shape=PIECES,
        compiler_params=pltpu.CompilerParams(vmem_limit_bytes=8 * 2**20),
        cost_estimate=pl.CostEstimate(flops=2**28, bytes_accessed=2**21, transcendentals=0),
        name="keep",
    )(facts, hidden, latent_grad_t, up_term, sums)


def halved(wide):
    high = wide.astype(jnp.bfloat16)
    return high, (wide - high.astype(jnp.float32)).astype(jnp.bfloat16)


def merge_kernel(kept, came, out_ref):
    row = lax.broadcasted_iota(jnp.int32, (8, HEAD_DIM), 0)
    for r in range(out_ref.shape[0]):
        out_ref[r, :32, :] = (kept[r, :32, :] + came[r, :32, :]).astype(jnp.bfloat16)
        rows = kept[r, 32:, :] + came[r, 32:, :]
        rest = rows - rows.astype(jnp.bfloat16).astype(jnp.float32)
        out_ref[r, 32:, :] = jnp.where(row == 5, pltpu.roll(rest, 1, 0), rows).astype(jnp.bfloat16)


def merged(kept, came):
    return pl.pallas_call(
        merge_kernel,
        out_shape=jax.ShapeDtypeStruct(PIECES.shape, jnp.bfloat16),
        compiler_params=SMALL,
        name="merge",
    )(kept, came)


def fold_kernel(pieces_ref, out_ref):
    total = jnp.sum(pieces_ref[...].astype(jnp.float32), axis=0)
    row = lax.broadcasted_iota(jnp.int32, (8, HEAD_DIM), 0)
    tail = total[32:, :]
    tail = jnp.where(row == 4, tail + pltpu.roll(tail, 7, 0), tail)
    high, low = halved(tail)
    rows = jnp.concatenate([total[:32, :].astype(jnp.bfloat16), jnp.concatenate([high, low], axis=0)], axis=0)
    for d in range(out_ref.shape[0]):
        out_ref[d] = rows


def fold(pieces, copies):
    return pl.pallas_call(
        fold_kernel,
        out_shape=jax.ShapeDtypeStruct((copies, PIECE_ROWS + 8, HEAD_DIM), jnp.bfloat16),
        compiler_params=SMALL,
        name="fold",
    )(pieces)


def owner_kernel(pieces_ref, down_ref, average_ref, grad_ref, next_ref, up_ref, loss_ref):
    total = jnp.sum(pieces_ref[...].astype(jnp.float32), axis=0)
    tail = total[32:40, :] + total[40:48, :]
    count = tail[4:5, 1:2]
    loss_ref[...] = tail[4:5, 0:1] / (2.0 * count)
    factor = adapter_scale / count
    rows = jnp.concatenate([total[:32, :RANK], total[:32, RANK:]], axis=0)
    grad = jnp.transpose(rows) * factor
    grad_ref[...] = grad
    next_ref[...] = average_decay * average_ref[...] + (1.0 - average_decay) * (down_ref[...] - learning_rate * grad)
    piece = tail[:4, :] * factor
    for d in range(up_ref.shape[0]):
        up_ref[d] = piece


def owner_update(pieces, down_map, average_down_map, copies):
    shape = jax.ShapeDtypeStruct
    return pl.pallas_call(
        owner_kernel,
        out_shape=[
            shape((RANK, RANK), jnp.float32),
            shape((RANK, RANK), jnp.float32),
            shape((copies, 4, HEAD_DIM), jnp.float32),
            shape((1, 1), jnp.float32),
        ],
        compiler_params=SMALL,
        name="owner",
    )(pieces, down_map, average_down_map)


def second_kernel(pieces_ref, up_ref, average_ref, grad_ref, next_ref):
    for j in range(MODEL // RANK):
        q, b = divmod(j // 2, 4)
        top = 8 * q + 4 * (j % 2)
        grad_ref[top : top + 4, b * 128 : (b + 1) * 128] = pieces_ref[j]
    next_ref[...] = average_decay * average_ref[...] + (1.0 - average_decay) * (
        up_ref[...] - learning_rate * grad_ref[...]
    )


def second_update(pieces, up_map, average_up_map):
    shape = jax.ShapeDtypeStruct((RANK, KV_WIDTH), jnp.float32)
    return pl.pallas_call(second_kernel, out_shape=[shape, shape], compiler_params=SMALL, name="second")(
        pieces, up_map, average_up_map
    )


def exchange(pieces, axis):
    return lax.all_to_all(pieces, axis, 0, 0, tiled=True)


def along_y(owners):
    return [list(range(k, owners, 8)) for k in range(8)]


def same_core(owners):
    return [list(range(core, owners, 2)) for core in range(2)]


def along_x(block, owners, shift):
    moved = [(i, i // 8 * 8 + (i + 2 * shift) % 8) for i in range(owners)]
    return lax.ppermute(block, "fsdp", moved)


def from_neighbour(part, owners, replicas, y, z):
    moved = [
        ((d + z) % replicas * owners + (i + 8 * y) % owners, d * owners + i)
        for d in range(replicas)
        for i in range(owners)
    ]
    return lax.ppermute(part, ("dp", "fsdp"), moved)


def from_other_core(block, owners):
    return lax.ppermute(block, "fsdp", [(i, i ^ 1) for i in range(owners)])


def per_device(
    hidden,
    queries,
    keys,
    target,
    lengths,
    value_weight_frozen,
    adapter_down_map,
    adapter_up_map,
    average_down_map,
    average_up_map,
):
    owners, replicas = lax.axis_size("fsdp"), lax.axis_size("dp")
    place = lax.axis_index("fsdp").astype(jnp.int32)
    plane = lax.axis_index("dp").astype(jnp.int32)
    quarter = (plane & 1) * 2 + ((place >> 3) & 1)
    facts = jnp.stack([lengths[0], place & 1, (place >> 1) & 3, quarter])
    shards = packed_shard(value_weight_frozen, adapter_down_map, owners // 8)
    own = lax.all_to_all(shards, "fsdp", 0, 0, tiled=True, axis_index_groups=along_y(owners))
    mine, send = split_hidden(facts, hidden)
    theirs = from_other_core(send, owners)
    probs, probs_t = attention_probs(lengths, queries, keys)
    part = along_x(lax.dynamic_slice_in_dim(own, quarter * 2, 2, axis=0), owners, 2)
    near = along_x(own, owners, 1)
    far = along_x(own, owners, 3)
    beside = from_neighbour(part, owners, replicas, 1, 0)
    behind = from_neighbour(part, owners, replicas, 0, 1)
    corner = from_neighbour(part, owners, replicas, 1, 1)
    total = None
    for shift, given in ((0, (own,)), (3, (far,)), (2, (part, beside, behind, corner))):
        total = partial_values(facts, mine, theirs, given, shift, total)
    total, other = partial_values(facts, mine, theirs, (near,), 1, total, last=True)
    swapped = from_other_core(other, owners)
    pieces, latent_grad_t, up_term, sums = gradients(
        facts, send, total, swapped, probs, probs_t, target, adapter_up_map
    )
    came = from_other_core(pieces, owners)
    kept = kept_pieces(facts, mine, latent_grad_t, up_term, sums)
    arrived = lax.all_to_all(
        merged(kept, came), "fsdp", 0, 0, tiled=True, axis_index_groups=same_core(owners)
    )
    summed = fold(arrived, replicas)
    down_grad, average_down_next, up_piece, loss = owner_update(
        exchange(summed, "dp"), adapter_down_map, average_down_map, owners
    )
    up_grad, average_up_next = second_update(exchange(up_piece, "fsdp"), adapter_up_map, average_up_map)
    return (down_grad, up_grad, average_down_next, average_up_next, loss.reshape(()))


def solution(mesh):
    placed = (
        P(("dp", "fsdp"), None),
        P(("dp", "fsdp"), None),
        P(("dp", "fsdp"), None),
        P(("dp", "fsdp"), None),
        P(("dp", "fsdp")),
        P("fsdp", None),
        P("fsdp", None),
        P(),
        P("fsdp", None),
        P(),
    )
    return jax.shard_map(
        per_device,
        mesh=mesh,
        in_specs=placed,
        out_specs=(P("fsdp", None), P(), P("fsdp", None), P(), P()),
        check_vma=False,
    )
```

```python
import math

import jax
import jax.numpy as jnp
from jax import lax
from jax.experimental import pallas as pl
from jax.experimental.pallas import tpu as pltpu
from jax.sharding import PartitionSpec as P


HEADS = 16
KEY_VALUE_HEADS = 4
HEAD_DIM = 128
GROUP = HEADS // KEY_VALUE_HEADS
TOK = 256
MODEL = 4096
RANK = 64
KV_WIDTH = KEY_VALUE_HEADS * HEAD_DIM
WIDTH = KV_WIDTH + RANK
PADDED = KV_WIDTH + HEAD_DIM

adapter_scale = 2.0
average_decay = 0.9
learning_rate = 1.0
masked_score = -1e30

PIECE_ROWS = 40
SMALL = pltpu.CompilerParams(vmem_limit_bytes=4 * 2**20)


def nt(a, b):
    return lax.dot_general(a, b, (((1,), (1,)), ((), ())), preferred_element_type=jnp.float32)


def nn(a, b):
    return lax.dot_general(a, b, (((1,), (0,)), ((), ())), preferred_element_type=jnp.float32)


def probs_kernel(length_ref, q_ref, k_ref, p_ref, pt_ref):
    length = length_ref[0]
    keys = k_ref[...]
    row = lax.broadcasted_iota(jnp.int32, (TOK, TOK), 0)
    col = lax.broadcasted_iota(jnp.int32, (TOK, TOK), 1)
    allowed = (col <= row) & (col < length)
    for g in range(GROUP):
        scores = nt(q_ref[:, g * HEAD_DIM : (g + 1) * HEAD_DIM], keys) * (1.0 / math.sqrt(HEAD_DIM))
        scores = jnp.where(allowed, scores, masked_score)
        weights = jnp.exp(scores - jnp.max(scores, axis=-1, keepdims=True))
        probs = weights * (1.0 / jnp.sum(weights, axis=-1, keepdims=True))
        p_ref[0, g * TOK : (g + 1) * TOK, :] = probs.astype(jnp.bfloat16)
        pt_ref[0, :, g * TOK : (g + 1) * TOK] = jnp.transpose(probs).astype(jnp.bfloat16)


def attention_probs(lengths, queries, keys):
    shape = jax.ShapeDtypeStruct
    return pl.pallas_call(
        probs_kernel,
        grid=(KEY_VALUE_HEADS,),
        in_specs=[
            pl.BlockSpec(memory_space=pltpu.SMEM),
            pl.BlockSpec((TOK, GROUP * HEAD_DIM), lambda h: (0, h)),
            pl.BlockSpec((TOK, HEAD_DIM), lambda h: (0, h)),
        ],
        out_specs=[
            pl.BlockSpec((1, GROUP * TOK, TOK), lambda h: (h, 0, 0)),
            pl.BlockSpec((1, TOK, GROUP * TOK), lambda h: (h, 0, 0)),
        ],
        out_shape=[
            shape((KEY_VALUE_HEADS, GROUP * TOK, TOK), jnp.bfloat16),
            shape((KEY_VALUE_HEADS, TOK, GROUP * TOK), jnp.bfloat16),
        ],
        compiler_params=pltpu.CompilerParams(vmem_limit_bytes=60 * 2**20),
        cost_estimate=pl.CostEstimate(flops=2**31, bytes_accessed=6 * 2**20, transcendentals=2**20),
        name="probs",
    )(lengths, queries, keys)


def pack_kernel(value_ref, down_ref, out_ref):
    down = down_ref[...].astype(jnp.bfloat16)
    for d in range(out_ref.shape[0]):
        out_ref[d, :, :KV_WIDTH] = value_ref[...]
        out_ref[d, :, KV_WIDTH:] = down


def packed_shard(value_rows, down_rows, copies):
    return pl.pallas_call(
        pack_kernel,
        out_shape=jax.ShapeDtypeStruct((copies, RANK, WIDTH), jnp.bfloat16),
        compiler_params=pltpu.CompilerParams(vmem_limit_bytes=67_000_000),
        name="pack",
    )(value_rows, down_rows)


def places():
    place, plane = lax.axis_index("fsdp"), lax.axis_index("dp")
    return place & 1, (place >> 1) & 3, (plane & 1) * 2 + ((place >> 3) & 1)


def split_kernel(hidden, keep, send):
    first = lax.broadcasted_iota(jnp.int32, (TOK, HEAD_DIM), 1) < RANK
    mine = places()[0] == 0
    for x in range(4):
        for y in range(0, 8, 2):
            a = hidden[:, y * 512 + x * 128 : y * 512 + (x + 1) * 128].astype(jnp.float32)
            b = hidden[:, (y + 1) * 512 + x * 128 : (y + 1) * 512 + (x + 1) * 128].astype(jnp.float32)
            even = jnp.where(first, a, pltpu.roll(b, RANK, 1))
            odd = jnp.where(first, pltpu.roll(a, RANK, 1), b)
            to = pl.ds(x * 512 + y * 64, 128)
            keep[:, to] = jnp.where(mine, even, odd).astype(jnp.bfloat16)
            send[:, to] = jnp.where(mine, odd, even).astype(jnp.bfloat16)


def split_hidden(hidden):
    vmem = pl.BlockSpec(memory_space=pltpu.VMEM)
    shape = jax.ShapeDtypeStruct((TOK, MODEL // 2), jnp.bfloat16)
    return pl.pallas_call(
        split_kernel,
        in_specs=[vmem],
        out_specs=[vmem, vmem],
        out_shape=[shape, shape],
        compiler_params=pltpu.CompilerParams(vmem_limit_bytes=12 * 2**20),
        cost_estimate=pl.CostEstimate(flops=2**30, bytes_accessed=2**22, transcendentals=0),
        name="split",
    )(hidden)


def block_product(tokens, block, which):
    _, x, own_quarter = places()
    column = ((x + (4 - which)) & 3) * 512
    if len(block) == 1:
        return nn(tokens[:, pl.ds(pl.multiple_of(column, 512), 512)], block[0][...].reshape(512, WIDTH))
    total = None
    for j in (0, 2):
        left, right = [], []
        for k in (j, j + 1):
            quarter = own_quarter ^ k
            left.append(tokens[:, pl.ds(pl.multiple_of(column + quarter * 128, 128), 128)])
            right.append(block[k][...].reshape(128, WIDTH))
        part = nn(jnp.concatenate(left, axis=1), jnp.concatenate(right, axis=0))
        total = part if total is None else total + part
    return total


def first_kernel(mine, theirs, own, out):
    for i, tokens in enumerate((mine, theirs)):
        out[i] = block_product(tokens, (own,), 0)


def next_kernel(mine, theirs, far, before, out):
    for i, tokens in enumerate((mine, theirs)):
        out[i] = block_product(tokens, (far,), 3) + before[i]


def last_kernel(mine, theirs, q0, q1, q2, q3, near, before, own, other):
    for i, (tokens, out) in enumerate(((mine, own), (theirs, other))):
        far = block_product(tokens, (q0, q1, q2, q3), 2)
        out[:, :WIDTH] = (before[i] + far) + block_product(tokens, (near,), 1)
        out[:, WIDTH:] = jnp.zeros((TOK, PADDED - WIDTH), jnp.float32)


def partial_values(body, *given):
    vmem = pl.BlockSpec(memory_space=pltpu.VMEM)
    shape = jax.ShapeDtypeStruct
    last = body is last_kernel
    return pl.pallas_call(
        body,
        in_specs=[vmem] * len(given),
        out_specs=[vmem, vmem] if last else vmem,
        out_shape=[shape((TOK, PADDED), jnp.float32)] * 2 if last else shape((2, TOK, WIDTH), jnp.float32),
        compiler_params=pltpu.CompilerParams(vmem_limit_bytes=12 * 2**20),
        cost_estimate=pl.CostEstimate(flops=2**29, bytes_accessed=2**21, transcendentals=0),
        name="partial",
    )(*given)


def store_pieces(out_ref, latent_grad_t, hidden, up_term, facts, core):
    lane = lax.broadcasted_iota(jnp.int32, (RANK // 2, HEAD_DIM), 1) < RANK
    for x in range(4):
        term = nn(latent_grad_t, hidden[:, x * 512 : (x + 1) * 512])
        for i in range(4):
            a = term[: RANK // 2, i * 128 : (i + 1) * 128]
            b = term[RANK // 2 :, i * 128 : (i + 1) * 128]
            out_ref[8 * i + x, :32, :] = jnp.where(lane, a, pltpu.roll(b, RANK, 1))
            out_ref[8 * i + 4 + x, :32, :] = jnp.where(lane, pltpu.roll(a, RANK, 1), b)
    sub = lax.broadcasted_iota(jnp.int32, (8, HEAD_DIM), 0)
    for q in range(8):
        for b in range(4):
            tile = up_term[8 * q : 8 * q + 8, b * 128 : (b + 1) * 128]
            rows = jnp.where(core == 0, tile, pltpu.roll(tile, 4, 0))
            out_ref[4 * q + b, 32:, :] = jnp.where(sub < 4, rows, facts)


def grads_kernel(
    length_ref, hidden, before, swapped, probs, probs_t, target, up_ref,
    out_ref, latent_grad_ref, up_term_ref, sums_ref, cot, value_grad,
):
    length = length_ref[0]
    up = up_ref[...].astype(jnp.bfloat16)
    total = before[...] + swapped[...]
    latent = total[:, KV_WIDTH:WIDTH].astype(jnp.bfloat16)
    values = (total[:, :KV_WIDTH] + adapter_scale * nn(latent, up)).astype(jnp.bfloat16)

    live = lax.broadcasted_iota(jnp.int32, (TOK, HEAD_DIM), 0) < length
    squares = jnp.zeros((TOK, HEAD_DIM), jnp.float32)
    for k in range(KEY_VALUE_HEADS):
        output = nn(probs[k], values[:, k * HEAD_DIM : (k + 1) * HEAD_DIM])
        for g in range(GROUP):
            h = k * GROUP + g
            aim = target[:, h * HEAD_DIM : (h + 1) * HEAD_DIM].astype(jnp.float32)
            differ = jnp.where(live, output[g * TOK : (g + 1) * TOK, :] - aim, 0.0)
            squares = squares + differ * differ
            cot[k, g * TOK : (g + 1) * TOK, :] = differ.astype(jnp.bfloat16)
        value_grad[:, k * HEAD_DIM : (k + 1) * HEAD_DIM] = nn(probs_t[k], cot[k]).astype(jnp.bfloat16)

    grad = value_grad[...]
    latent_grad_t = nt(up, grad).astype(jnp.bfloat16)
    up_term = lax.dot_general(latent, grad, (((0,), (0,)), ((), ())), preferred_element_type=jnp.float32)

    loss = jnp.sum(jnp.sum(squares, axis=0, keepdims=True), axis=1, keepdims=True)
    lane = lax.broadcasted_iota(jnp.int32, (8, HEAD_DIM), 1)
    row = lax.broadcasted_iota(jnp.int32, (8, HEAD_DIM), 0)
    count = jnp.full((8, HEAD_DIM), length, jnp.int32).astype(jnp.float32)
    sums = jnp.where(lane == 0, loss, jnp.where(lane == 1, count, 0.0))
    sums = jnp.where(row == 4, sums, 0.0)
    latent_grad_ref[...] = latent_grad_t
    up_term_ref[...] = up_term
    sums_ref[...] = sums
    store_pieces(out_ref, latent_grad_t, hidden, up_term, sums, 1 - places()[0])


PIECES = jax.ShapeDtypeStruct((MODEL // RANK // 2, PIECE_ROWS, HEAD_DIM), jnp.float32)


def gradients(lengths, hidden, before, swapped, probs, probs_t, target, up_map):
    vmem = pl.BlockSpec(memory_space=pltpu.VMEM)
    shape = jax.ShapeDtypeStruct
    return pl.pallas_call(
        grads_kernel,
        in_specs=[pl.BlockSpec(memory_space=pltpu.SMEM)] + [vmem] * 7,
        out_specs=[vmem] * 4,
        out_shape=[
            PIECES,
            shape((RANK, TOK), jnp.bfloat16),
            shape((RANK, KV_WIDTH), jnp.float32),
            shape((8, HEAD_DIM), jnp.float32),
        ],
        scratch_shapes=[
            pltpu.VMEM((KEY_VALUE_HEADS, GROUP * TOK, HEAD_DIM), jnp.bfloat16),
            pltpu.VMEM((TOK, KV_WIDTH), jnp.bfloat16),
        ],
        compiler_params=pltpu.CompilerParams(vmem_limit_bytes=24 * 2**20),
        cost_estimate=pl.CostEstimate(flops=2**32, bytes_accessed=10 * 2**20, transcendentals=0),
        name="grads",
    )(lengths, hidden, before, swapped, probs, probs_t, target, up_map)


def keep_kernel(hidden, latent_grad_ref, up_term_ref, sums_ref, out_ref):
    store_pieces(out_ref, latent_grad_ref[...], hidden, up_term_ref[...], sums_ref[...], places()[0])


def kept_pieces(hidden, latent_grad_t, up_term, sums):
    vmem = pl.BlockSpec(memory_space=pltpu.VMEM)
    return pl.pallas_call(
        keep_kernel,
        in_specs=[vmem] * 4,
        out_specs=vmem,
        out_shape=PIECES,
        compiler_params=pltpu.CompilerParams(vmem_limit_bytes=8 * 2**20),
        cost_estimate=pl.CostEstimate(flops=2**28, bytes_accessed=2**21, transcendentals=0),
        name="keep",
    )(hidden, latent_grad_t, up_term, sums)


def halved(wide):
    high = wide.astype(jnp.bfloat16)
    return high, (wide - high.astype(jnp.float32)).astype(jnp.bfloat16)


def merge_kernel(kept, came, out_ref):
    row = lax.broadcasted_iota(jnp.int32, (8, HEAD_DIM), 0)
    for r in range(out_ref.shape[0]):
        out_ref[r, :32, :] = (kept[r, :32, :] + came[r, :32, :]).astype(jnp.bfloat16)
        rows = kept[r, 32:, :] + came[r, 32:, :]
        rest = rows - rows.astype(jnp.bfloat16).astype(jnp.float32)
        out_ref[r, 32:, :] = jnp.where(row == 5, pltpu.roll(rest, 1, 0), rows).astype(jnp.bfloat16)


def merged(kept, came):
    return pl.pallas_call(
        merge_kernel,
        out_shape=jax.ShapeDtypeStruct(PIECES.shape, jnp.bfloat16),
        compiler_params=SMALL,
        name="merge",
    )(kept, came)


def fold_kernel(pieces_ref, out_ref):
    total = jnp.sum(pieces_ref[...].astype(jnp.float32), axis=0)
    row = lax.broadcasted_iota(jnp.int32, (8, HEAD_DIM), 0)
    tail = total[32:, :]
    tail = jnp.where(row == 4, tail + pltpu.roll(tail, 7, 0), tail)
    high, low = halved(tail)
    rows = jnp.concatenate([total[:32, :].astype(jnp.bfloat16), jnp.concatenate([high, low], axis=0)], axis=0)
    for d in range(out_ref.shape[0]):
        out_ref[d] = rows


def fold(pieces, copies):
    return pl.pallas_call(
        fold_kernel,
        out_shape=jax.ShapeDtypeStruct((copies, PIECE_ROWS + 8, HEAD_DIM), jnp.bfloat16),
        compiler_params=SMALL,
        name="fold",
    )(pieces)


def owner_kernel(pieces_ref, down_ref, average_ref, grad_ref, next_ref, up_ref, loss_ref):
    total = jnp.sum(pieces_ref[...].astype(jnp.float32), axis=0)
    tail = total[32:40, :] + total[40:48, :]
    count = tail[4:5, 1:2]
    loss_ref[...] = tail[4:5, 0:1] / (2.0 * count)
    factor = adapter_scale / count
    rows = jnp.concatenate([total[:32, :RANK], total[:32, RANK:]], axis=0)
    grad = jnp.transpose(rows) * factor
    grad_ref[...] = grad
    next_ref[...] = average_decay * average_ref[...] + (1.0 - average_decay) * (down_ref[...] - learning_rate * grad)
    piece = tail[:4, :] * factor
    for d in range(up_ref.shape[0]):
        up_ref[d] = piece


def owner_update(pieces, down_map, average_down_map, copies):
    shape = jax.ShapeDtypeStruct
    return pl.pallas_call(
        owner_kernel,
        out_shape=[
            shape((RANK, RANK), jnp.float32),
            shape((RANK, RANK), jnp.float32),
            shape((copies, 4, HEAD_DIM), jnp.float32),
            shape((1, 1), jnp.float32),
        ],
        compiler_params=SMALL,
        name="owner",
    )(pieces, down_map, average_down_map)


def second_kernel(pieces_ref, up_ref, average_ref, grad_ref, next_ref):
    for j in range(MODEL // RANK):
        q, b = divmod(j // 2, 4)
        top = 8 * q + 4 * (j % 2)
        grad_ref[top : top + 4, b * 128 : (b + 1) * 128] = pieces_ref[j]
    next_ref[...] = average_decay * average_ref[...] + (1.0 - average_decay) * (
        up_ref[...] - learning_rate * grad_ref[...]
    )


def second_update(pieces, up_map, average_up_map):
    shape = jax.ShapeDtypeStruct((RANK, KV_WIDTH), jnp.float32)
    return pl.pallas_call(second_kernel, out_shape=[shape, shape], compiler_params=SMALL, name="second")(
        pieces, up_map, average_up_map
    )


def exchange(pieces, axis):
    return lax.all_to_all(pieces, axis, 0, 0, tiled=True)


def along_y(owners):
    return [list(range(k, owners, 8)) for k in range(8)]


def same_core(owners):
    return [list(range(core, owners, 2)) for core in range(2)]


def along_x(block, owners, shift):
    moved = [(i, i // 8 * 8 + (i + 2 * shift) % 8) for i in range(owners)]
    return lax.ppermute(block, "fsdp", moved)


def from_neighbour(part, owners, replicas, y, z):
    moved = [
        ((d + z) % replicas * owners + (i + 8 * y) % owners, d * owners + i)
        for d in range(replicas)
        for i in range(owners)
    ]
    return lax.ppermute(part, ("dp", "fsdp"), moved)


def from_other_core(block, owners):
    return lax.ppermute(block, "fsdp", [(i, i ^ 1) for i in range(owners)])


def per_device(
    hidden,
    queries,
    keys,
    target,
    lengths,
    value_weight_frozen,
    adapter_down_map,
    adapter_up_map,
    average_down_map,
    average_up_map,
):
    owners, replicas = lax.axis_size("fsdp"), lax.axis_size("dp")
    quarter = places()[2]
    shards = packed_shard(value_weight_frozen, adapter_down_map, owners // 8)
    own = lax.all_to_all(shards, "fsdp", 0, 0, tiled=True, axis_index_groups=along_y(owners))
    mine, send = split_hidden(hidden)
    theirs = from_other_core(send, owners)
    probs, probs_t = attention_probs(lengths, queries, keys)
    part = along_x(lax.dynamic_slice_in_dim(own, quarter * 2, 2, axis=0), owners, 2)
    near = along_x(own, owners, 1)
    far = along_x(own, owners, 3)
    beside = from_neighbour(part, owners, replicas, 1, 0)
    behind = from_neighbour(part, owners, replicas, 0, 1)
    corner = from_neighbour(part, owners, replicas, 1, 1)
    total = partial_values(first_kernel, mine, theirs, own)
    total = partial_values(next_kernel, mine, theirs, far, total)
    total, other = partial_values(
        last_kernel, mine, theirs, part, beside, behind, corner, near, total
    )
    swapped = from_other_core(other, owners)
    pieces, latent_grad_t, up_term, sums = gradients(
        lengths, send, total, swapped, probs, probs_t, target, adapter_up_map
    )
    came = from_other_core(pieces, owners)
    kept = kept_pieces(mine, latent_grad_t, up_term, sums)
    arrived = lax.all_to_all(
        merged(kept, came), "fsdp", 0, 0, tiled=True, axis_index_groups=same_core(owners)
    )
    summed = fold(arrived, replicas)
    down_grad, average_down_next, up_piece, loss = owner_update(
        exchange(summed, "dp"), adapter_down_map, average_down_map, owners
    )
    up_grad, average_up_next = second_update(exchange(up_piece, "fsdp"), adapter_up_map, average_up_map)
    return (down_grad, up_grad, average_down_next, average_up_next, loss.reshape(()))


def solution(mesh):
    placed = (
        P(("dp", "fsdp"), None),
        P(("dp", "fsdp"), None),
        P(("dp", "fsdp"), None),
        P(("dp", "fsdp"), None),
        P(("dp", "fsdp")),
        P("fsdp", None),
        P("fsdp", None),
        P(),
        P("fsdp", None),
        P(),
    )
    return jax.shard_map(
        per_device,
        mesh=mesh,
        in_specs=placed,
        out_specs=(P("fsdp", None), P(), P("fsdp", None), P(), P()),
        check_vma=False,
    )
```

```python
import math

import jax
import jax.numpy as jnp
from jax import lax
from jax.experimental import pallas as pl
from jax.experimental.pallas import tpu as pltpu
from jax.sharding import PartitionSpec as P


HEADS = 16
KEY_VALUE_HEADS = 4
HEAD_DIM = 128
GROUP = HEADS // KEY_VALUE_HEADS
TOK = 256
MODEL = 4096
RANK = 64
KV_WIDTH = KEY_VALUE_HEADS * HEAD_DIM
WIDTH = KV_WIDTH + RANK
PADDED = KV_WIDTH + HEAD_DIM

adapter_scale = 2.0
average_decay = 0.9
learning_rate = 1.0
masked_score = -1e30

PIECE_ROWS = 40
SMALL = pltpu.CompilerParams(vmem_limit_bytes=4 * 2**20)


def nt(a, b):
    return lax.dot_general(a, b, (((1,), (1,)), ((), ())), preferred_element_type=jnp.float32)


def nn(a, b):
    return lax.dot_general(a, b, (((1,), (0,)), ((), ())), preferred_element_type=jnp.float32)


def probs_kernel(length_ref, q_ref, k_ref, p_ref, pt_ref):
    length = length_ref[0]
    keys = k_ref[...]
    row = lax.broadcasted_iota(jnp.int32, (TOK, TOK), 0)
    col = lax.broadcasted_iota(jnp.int32, (TOK, TOK), 1)
    allowed = (col <= row) & (col < length)
    for g in range(GROUP):
        scores = nt(q_ref[:, g * HEAD_DIM : (g + 1) * HEAD_DIM], keys) * (1.0 / math.sqrt(HEAD_DIM))
        scores = jnp.where(allowed, scores, masked_score)
        weights = jnp.exp(scores - jnp.max(scores, axis=-1, keepdims=True))
        probs = weights * (1.0 / jnp.sum(weights, axis=-1, keepdims=True))
        p_ref[0, g * TOK : (g + 1) * TOK, :] = probs.astype(jnp.bfloat16)
        pt_ref[0, :, g * TOK : (g + 1) * TOK] = jnp.transpose(probs).astype(jnp.bfloat16)


def attention_probs(lengths, queries, keys):
    shape = jax.ShapeDtypeStruct
    return pl.pallas_call(
        probs_kernel,
        grid=(KEY_VALUE_HEADS,),
        in_specs=[
            pl.BlockSpec(memory_space=pltpu.SMEM),
            pl.BlockSpec((TOK, GROUP * HEAD_DIM), lambda h: (0, h)),
            pl.BlockSpec((TOK, HEAD_DIM), lambda h: (0, h)),
        ],
        out_specs=[
            pl.BlockSpec((1, GROUP * TOK, TOK), lambda h: (h, 0, 0)),
            pl.BlockSpec((1, TOK, GROUP * TOK), lambda h: (h, 0, 0)),
        ],
        out_shape=[
            shape((KEY_VALUE_HEADS, GROUP * TOK, TOK), jnp.bfloat16),
            shape((KEY_VALUE_HEADS, TOK, GROUP * TOK), jnp.bfloat16),
        ],
        compiler_params=pltpu.CompilerParams(vmem_limit_bytes=60 * 2**20),
        cost_estimate=pl.CostEstimate(flops=2**31, bytes_accessed=6 * 2**20, transcendentals=2**20),
        name="probs",
    )(lengths, queries, keys)


def pack_kernel(value_ref, down_ref, out_ref):
    down = down_ref[...].astype(jnp.bfloat16)
    for d in range(out_ref.shape[0]):
        out_ref[d, :, :KV_WIDTH] = value_ref[...]
        out_ref[d, :, KV_WIDTH:] = down


def packed_shard(value_rows, down_rows, copies):
    return pl.pallas_call(
        pack_kernel,
        out_shape=jax.ShapeDtypeStruct((copies, RANK, WIDTH), jnp.bfloat16),
        compiler_params=pltpu.CompilerParams(vmem_limit_bytes=67_000_000),
        name="pack",
    )(value_rows, down_rows)


def places():
    place, plane = lax.axis_index("fsdp"), lax.axis_index("dp")
    return place & 1, (place >> 1) & 3, (plane & 1) * 2 + ((place >> 3) & 1)


def split_kernel(hidden, keep, send):
    first = lax.broadcasted_iota(jnp.int32, (TOK, HEAD_DIM), 1) < RANK
    mine = places()[0] == 0
    for x in range(4):
        for y in range(0, 8, 2):
            a = hidden[:, y * 512 + x * 128 : y * 512 + (x + 1) * 128].astype(jnp.float32)
            b = hidden[:, (y + 1) * 512 + x * 128 : (y + 1) * 512 + (x + 1) * 128].astype(jnp.float32)
            even = jnp.where(first, a, pltpu.roll(b, RANK, 1))
            odd = jnp.where(first, pltpu.roll(a, RANK, 1), b)
            to = pl.ds(x * 512 + y * 64, 128)
            keep[:, to] = jnp.where(mine, even, odd).astype(jnp.bfloat16)
            send[:, to] = jnp.where(mine, odd, even).astype(jnp.bfloat16)


def split_hidden(hidden):
    vmem = pl.BlockSpec(memory_space=pltpu.VMEM)
    shape = jax.ShapeDtypeStruct((TOK, MODEL // 2), jnp.bfloat16)
    return pl.pallas_call(
        split_kernel,
        in_specs=[vmem],
        out_specs=[vmem, vmem],
        out_shape=[shape, shape],
        compiler_params=pltpu.CompilerParams(vmem_limit_bytes=12 * 2**20),
        cost_estimate=pl.CostEstimate(flops=2**30, bytes_accessed=2**22, transcendentals=0),
        name="split",
    )(hidden)


def block_product(tokens, block, which):
    _, x, own_quarter = places()
    column = ((x + (4 - which)) & 3) * 512
    if len(block) == 1:
        return nn(tokens[:, pl.ds(pl.multiple_of(column, 512), 512)], block[0][...].reshape(512, WIDTH))
    total = None
    for j in (0, 2):
        left, right = [], []
        for k in (j, j + 1):
            quarter = own_quarter ^ k
            left.append(tokens[:, pl.ds(pl.multiple_of(column + quarter * 128, 128), 128)])
            right.append(block[k][...].reshape(128, WIDTH))
        part = nn(jnp.concatenate(left, axis=1), jnp.concatenate(right, axis=0))
        total = part if total is None else total + part
    return total


def first_kernel(mine, theirs, own, out):
    for i, tokens in enumerate((mine, theirs)):
        out[i] = block_product(tokens, (own,), 0)


def next_kernel(mine, theirs, far, before, out):
    for i, tokens in enumerate((mine, theirs)):
        out[i] = block_product(tokens, (far,), 3) + before[i]


def last_kernel(mine, theirs, q0, q1, q2, q3, near, before, own, other):
    for i, (tokens, out) in enumerate(((mine, own), (theirs, other))):
        far = block_product(tokens, (q0, q1, q2, q3), 2)
        out[:, :WIDTH] = (before[i] + far) + block_product(tokens, (near,), 1)
        out[:, WIDTH:] = jnp.zeros((TOK, PADDED - WIDTH), jnp.float32)


def partial_values(body, *given):
    vmem = pl.BlockSpec(memory_space=pltpu.VMEM)
    shape = jax.ShapeDtypeStruct
    last = body is last_kernel
    return pl.pallas_call(
        body,
        in_specs=[vmem] * len(given),
        out_specs=[vmem, vmem] if last else vmem,
        out_shape=[shape((TOK, PADDED), jnp.float32)] * 2 if last else shape((2, TOK, WIDTH), jnp.float32),
        compiler_params=pltpu.CompilerParams(vmem_limit_bytes=12 * 2**20),
        cost_estimate=pl.CostEstimate(flops=2**29, bytes_accessed=2**21, transcendentals=0),
        name="partial",
    )(*given)


def store_pieces(out_ref, latent_grad_t, hidden, up_term, facts, core):
    lane = lax.broadcasted_iota(jnp.int32, (RANK // 2, HEAD_DIM), 1) < RANK
    for x in range(4):
        term = nn(latent_grad_t, hidden[:, x * 512 : (x + 1) * 512])
        for i in range(4):
            a = term[: RANK // 2, i * 128 : (i + 1) * 128]
            b = term[RANK // 2 :, i * 128 : (i + 1) * 128]
            out_ref[8 * i + x, :32, :] = jnp.where(lane, a, pltpu.roll(b, RANK, 1))
            out_ref[8 * i + 4 + x, :32, :] = jnp.where(lane, pltpu.roll(a, RANK, 1), b)
    sub = lax.broadcasted_iota(jnp.int32, (8, HEAD_DIM), 0)
    for q in range(8):
        for b in range(4):
            tile = up_term[8 * q : 8 * q + 8, b * 128 : (b + 1) * 128]
            rows = jnp.where(core == 0, tile, pltpu.roll(tile, 4, 0))
            out_ref[4 * q + b, 32:, :] = jnp.where(sub < 4, rows, facts)


def grads_kernel(
    length_ref, hidden, before, swapped, probs, probs_t, target, up_ref,
    out_ref, latent_grad_ref, up_term_ref, sums_ref, cot, value_grad,
):
    length = length_ref[0]
    up = up_ref[...].astype(jnp.bfloat16)
    total = before[...] + swapped[...]
    latent = total[:, KV_WIDTH:WIDTH].astype(jnp.bfloat16)
    values = (total[:, :KV_WIDTH] + adapter_scale * nn(latent, up)).astype(jnp.bfloat16)

    live = lax.broadcasted_iota(jnp.int32, (TOK, HEAD_DIM), 0) < length
    squares = jnp.zeros((TOK, HEAD_DIM), jnp.float32)
    outputs = [nn(probs[k], values[:, k * HEAD_DIM : (k + 1) * HEAD_DIM]) for k in range(KEY_VALUE_HEADS)]
    for k in range(KEY_VALUE_HEADS):
        for g in range(GROUP):
            h = k * GROUP + g
            aim = target[:, h * HEAD_DIM : (h + 1) * HEAD_DIM].astype(jnp.float32)
            differ = jnp.where(live, outputs[k][g * TOK : (g + 1) * TOK, :] - aim, 0.0)
            squares = squares + differ * differ
            cot[k, g * TOK : (g + 1) * TOK, :] = differ.astype(jnp.bfloat16)
    for k in range(KEY_VALUE_HEADS):
        value_grad[:, k * HEAD_DIM : (k + 1) * HEAD_DIM] = nn(probs_t[k], cot[k]).astype(jnp.bfloat16)

    grad = value_grad[...]
    latent_grad_t = nt(up, grad).astype(jnp.bfloat16)
    up_term = lax.dot_general(latent, grad, (((0,), (0,)), ((), ())), preferred_element_type=jnp.float32)

    loss = jnp.sum(jnp.sum(squares, axis=0, keepdims=True), axis=1, keepdims=True)
    lane = lax.broadcasted_iota(jnp.int32, (8, HEAD_DIM), 1)
    row = lax.broadcasted_iota(jnp.int32, (8, HEAD_DIM), 0)
    count = jnp.full((8, HEAD_DIM), length, jnp.int32).astype(jnp.float32)
    sums = jnp.where(lane == 0, loss, jnp.where(lane == 1, count, 0.0))
    sums = jnp.where(row == 4, sums, 0.0)
    latent_grad_ref[...] = latent_grad_t
    up_term_ref[...] = up_term
    sums_ref[...] = sums
    store_pieces(out_ref, latent_grad_t, hidden, up_term, sums, 1 - places()[0])


PIECES = jax.ShapeDtypeStruct((MODEL // RANK // 2, PIECE_ROWS, HEAD_DIM), jnp.float32)


def gradients(lengths, hidden, before, swapped, probs, probs_t, target, up_map):
    vmem = pl.BlockSpec(memory_space=pltpu.VMEM)
    shape = jax.ShapeDtypeStruct
    return pl.pallas_call(
        grads_kernel,
        in_specs=[pl.BlockSpec(memory_space=pltpu.SMEM)] + [vmem] * 7,
        out_specs=[vmem] * 4,
        out_shape=[
            PIECES,
            shape((RANK, TOK), jnp.bfloat16),
            shape((RANK, KV_WIDTH), jnp.float32),
            shape((8, HEAD_DIM), jnp.float32),
        ],
        scratch_shapes=[
            pltpu.VMEM((KEY_VALUE_HEADS, GROUP * TOK, HEAD_DIM), jnp.bfloat16),
            pltpu.VMEM((TOK, KV_WIDTH), jnp.bfloat16),
        ],
        compiler_params=pltpu.CompilerParams(vmem_limit_bytes=24 * 2**20),
        cost_estimate=pl.CostEstimate(flops=2**32, bytes_accessed=10 * 2**20, transcendentals=0),
        name="grads",
    )(lengths, hidden, before, swapped, probs, probs_t, target, up_map)


def keep_kernel(hidden, latent_grad_ref, up_term_ref, sums_ref, out_ref):
    store_pieces(out_ref, latent_grad_ref[...], hidden, up_term_ref[...], sums_ref[...], places()[0])


def kept_pieces(hidden, latent_grad_t, up_term, sums):
    vmem = pl.BlockSpec(memory_space=pltpu.VMEM)
    return pl.pallas_call(
        keep_kernel,
        in_specs=[vmem] * 4,
        out_specs=vmem,
        out_shape=PIECES,
        compiler_params=pltpu.CompilerParams(vmem_limit_bytes=8 * 2**20),
        cost_estimate=pl.CostEstimate(flops=2**28, bytes_accessed=2**21, transcendentals=0),
        name="keep",
    )(hidden, latent_grad_t, up_term, sums)


def halved(wide):
    high = wide.astype(jnp.bfloat16)
    return high, (wide - high.astype(jnp.float32)).astype(jnp.bfloat16)


def merge_kernel(kept, came, out_ref):
    row = lax.broadcasted_iota(jnp.int32, (8, HEAD_DIM), 0)
    for r in range(out_ref.shape[0]):
        out_ref[r, :32, :] = (kept[r, :32, :] + came[r, :32, :]).astype(jnp.bfloat16)
        rows = kept[r, 32:, :] + came[r, 32:, :]
        rest = rows - rows.astype(jnp.bfloat16).astype(jnp.float32)
        out_ref[r, 32:, :] = jnp.where(row == 5, pltpu.roll(rest, 1, 0), rows).astype(jnp.bfloat16)


def merged(kept, came):
    return pl.pallas_call(
        merge_kernel,
        out_shape=jax.ShapeDtypeStruct(PIECES.shape, jnp.bfloat16),
        compiler_params=SMALL,
        name="merge",
    )(kept, came)


def fold_kernel(pieces_ref, out_ref):
    total = jnp.sum(pieces_ref[...].astype(jnp.float32), axis=0)
    row = lax.broadcasted_iota(jnp.int32, (8, HEAD_DIM), 0)
    tail = total[32:, :]
    tail = jnp.where(row == 4, tail + pltpu.roll(tail, 7, 0), tail)
    high, low = halved(tail)
    rows = jnp.concatenate([total[:32, :].astype(jnp.bfloat16), jnp.concatenate([high, low], axis=0)], axis=0)
    for d in range(out_ref.shape[0]):
        out_ref[d] = rows


def fold(pieces, copies):
    return pl.pallas_call(
        fold_kernel,
        out_shape=jax.ShapeDtypeStruct((copies, PIECE_ROWS + 8, HEAD_DIM), jnp.bfloat16),
        compiler_params=SMALL,
        name="fold",
    )(pieces)


def owner_kernel(pieces_ref, down_ref, average_ref, grad_ref, next_ref, up_ref, loss_ref):
    total = jnp.sum(pieces_ref[...].astype(jnp.float32), axis=0)
    tail = total[32:40, :] + total[40:48, :]
    count = tail[4:5, 1:2]
    loss_ref[...] = tail[4:5, 0:1] / (2.0 * count)
    factor = adapter_scale / count
    rows = jnp.concatenate([total[:32, :RANK], total[:32, RANK:]], axis=0)
    grad = jnp.transpose(rows) * factor
    grad_ref[...] = grad
    next_ref[...] = average_decay * average_ref[...] + (1.0 - average_decay) * (down_ref[...] - learning_rate * grad)
    piece = (tail[:4, :] * factor).astype(jnp.bfloat16)
    for d in range(up_ref.shape[0]):
        up_ref[d] = piece


def owner_update(pieces, down_map, average_down_map, copies):
    shape = jax.ShapeDtypeStruct
    return pl.pallas_call(
        owner_kernel,
        out_shape=[
            shape((RANK, RANK), jnp.float32),
            shape((RANK, RANK), jnp.float32),
            shape((copies, 4, HEAD_DIM), jnp.bfloat16),
            shape((1, 1), jnp.float32),
        ],
        compiler_params=SMALL,
        name="owner",
    )(pieces, down_map, average_down_map)


def second_kernel(pieces_ref, up_ref, average_ref, grad_ref, next_ref):
    for j in range(MODEL // RANK):
        q, b = divmod(j // 2, 4)
        top = 8 * q + 4 * (j % 2)
        grad_ref[top : top + 4, b * 128 : (b + 1) * 128] = pieces_ref[j].astype(jnp.float32)
    next_ref[...] = average_decay * average_ref[...] + (1.0 - average_decay) * (
        up_ref[...] - learning_rate * grad_ref[...]
    )


def second_update(pieces, up_map, average_up_map):
    shape = jax.ShapeDtypeStruct((RANK, KV_WIDTH), jnp.float32)
    return pl.pallas_call(second_kernel, out_shape=[shape, shape], compiler_params=SMALL, name="second")(
        pieces, up_map, average_up_map
    )


def exchange(pieces, axis):
    return lax.all_to_all(pieces, axis, 0, 0, tiled=True)


def along_y(owners):
    return [list(range(k, owners, 8)) for k in range(8)]


def same_core(owners):
    return [list(range(core, owners, 2)) for core in range(2)]


def along_x(block, owners, shift):
    moved = [(i, i // 8 * 8 + (i + 2 * shift) % 8) for i in range(owners)]
    return lax.ppermute(block, "fsdp", moved)


def from_neighbour(part, owners, replicas, y, z):
    moved = [
        ((d + z) % replicas * owners + (i + 8 * y) % owners, d * owners + i)
        for d in range(replicas)
        for i in range(owners)
    ]
    return lax.ppermute(part, ("dp", "fsdp"), moved)


def from_other_core(block, owners):
    return lax.ppermute(block, "fsdp", [(i, i ^ 1) for i in range(owners)])


def per_device(
    hidden,
    queries,
    keys,
    target,
    lengths,
    value_weight_frozen,
    adapter_down_map,
    adapter_up_map,
    average_down_map,
    average_up_map,
):
    owners, replicas = lax.axis_size("fsdp"), lax.axis_size("dp")
    quarter = places()[2]
    shards = packed_shard(value_weight_frozen, adapter_down_map, owners // 8)
    own = lax.all_to_all(shards, "fsdp", 0, 0, tiled=True, axis_index_groups=along_y(owners))
    mine, send = split_hidden(hidden)
    theirs = from_other_core(send, owners)
    probs, probs_t = attention_probs(lengths, queries, keys)
    part = along_x(lax.dynamic_slice_in_dim(own, quarter * 2, 2, axis=0), owners, 2)
    near = along_x(own, owners, 1)
    far = along_x(own, owners, 3)
    beside = from_neighbour(part, owners, replicas, 1, 0)
    behind = from_neighbour(part, owners, replicas, 0, 1)
    corner = from_neighbour(part, owners, replicas, 1, 1)
    total = partial_values(first_kernel, mine, theirs, own)
    total = partial_values(next_kernel, mine, theirs, far, total)
    total, other = partial_values(
        last_kernel, mine, theirs, part, beside, behind, corner, near, total
    )
    swapped = from_other_core(other, owners)
    pieces, latent_grad_t, up_term, sums = gradients(
        lengths, send, total, swapped, probs, probs_t, target, adapter_up_map
    )
    came = from_other_core(pieces, owners)
    kept = kept_pieces(mine, latent_grad_t, up_term, sums)
    arrived = lax.all_to_all(
        merged(kept, came), "fsdp", 0, 0, tiled=True, axis_index_groups=same_core(owners)
    )
    summed = fold(arrived, replicas)
    down_grad, average_down_next, up_piece, loss = owner_update(
        exchange(summed, "dp"), adapter_down_map, average_down_map, owners
    )
    up_grad, average_up_next = second_update(exchange(up_piece, "fsdp"), adapter_up_map, average_up_map)
    return (down_grad, up_grad, average_down_next, average_up_next, loss.reshape(()))


def solution(mesh):
    placed = (
        P(("dp", "fsdp"), None),
        P(("dp", "fsdp"), None),
        P(("dp", "fsdp"), None),
        P(("dp", "fsdp"), None),
        P(("dp", "fsdp")),
        P("fsdp", None),
        P("fsdp", None),
        P(),
        P("fsdp", None),
        P(),
    )
    return jax.shard_map(
        per_device,
        mesh=mesh,
        in_specs=placed,
        out_specs=(P("fsdp", None), P(), P("fsdp", None), P(), P()),
        check_vma=False,
    )
```

```python
import math

import jax
import jax.numpy as jnp
from jax import lax
from jax.experimental import pallas as pl
from jax.experimental.pallas import tpu as pltpu
from jax.sharding import PartitionSpec as P


HEADS = 16
KEY_VALUE_HEADS = 4
HEAD_DIM = 128
GROUP = HEADS // KEY_VALUE_HEADS
TOK = 256
MODEL = 4096
RANK = 64
KV_WIDTH = KEY_VALUE_HEADS * HEAD_DIM
WIDTH = KV_WIDTH + RANK
PADDED = KV_WIDTH + HEAD_DIM

adapter_scale = 2.0
average_decay = 0.9
learning_rate = 1.0
masked_score = -1e30

PIECE_ROWS = 40
SMALL = pltpu.CompilerParams(vmem_limit_bytes=4 * 2**20)


def nt(a, b):
    return lax.dot_general(a, b, (((1,), (1,)), ((), ())), preferred_element_type=jnp.float32)


def nn(a, b):
    return lax.dot_general(a, b, (((1,), (0,)), ((), ())), preferred_element_type=jnp.float32)


def probs_kernel(length_ref, q_ref, k_ref, p_ref, pt_ref):
    length = length_ref[0]
    keys = k_ref[...]
    row = lax.broadcasted_iota(jnp.int32, (TOK, TOK), 0)
    col = lax.broadcasted_iota(jnp.int32, (TOK, TOK), 1)
    allowed = (col <= row) & (col < length)
    for g in range(GROUP):
        scores = nt(q_ref[:, g * HEAD_DIM : (g + 1) * HEAD_DIM], keys) * (1.0 / math.sqrt(HEAD_DIM))
        scores = jnp.where(allowed, scores, masked_score)
        weights = jnp.exp(scores - jnp.max(scores, axis=-1, keepdims=True))
        probs = weights * (1.0 / jnp.sum(weights, axis=-1, keepdims=True))
        p_ref[0, g * TOK : (g + 1) * TOK, :] = probs.astype(jnp.bfloat16)
        pt_ref[0, :, g * TOK : (g + 1) * TOK] = jnp.transpose(probs).astype(jnp.bfloat16)


def attention_probs(lengths, queries, keys):
    shape = jax.ShapeDtypeStruct
    return pl.pallas_call(
        probs_kernel,
        grid=(KEY_VALUE_HEADS,),
        in_specs=[
            pl.BlockSpec(memory_space=pltpu.SMEM),
            pl.BlockSpec((TOK, GROUP * HEAD_DIM), lambda h: (0, h)),
            pl.BlockSpec((TOK, HEAD_DIM), lambda h: (0, h)),
        ],
        out_specs=[
            pl.BlockSpec((1, GROUP * TOK, TOK), lambda h: (h, 0, 0)),
            pl.BlockSpec((1, TOK, GROUP * TOK), lambda h: (h, 0, 0)),
        ],
        out_shape=[
            shape((KEY_VALUE_HEADS, GROUP * TOK, TOK), jnp.bfloat16),
            shape((KEY_VALUE_HEADS, TOK, GROUP * TOK), jnp.bfloat16),
        ],
        compiler_params=pltpu.CompilerParams(vmem_limit_bytes=60 * 2**20),
        cost_estimate=pl.CostEstimate(flops=2**31, bytes_accessed=6 * 2**20, transcendentals=2**20),
        name="probs",
    )(lengths, queries, keys)


def pack_kernel(value_ref, down_ref, out_ref):
    down = down_ref[...].astype(jnp.bfloat16)
    for d in range(out_ref.shape[0]):
        out_ref[d, :, :KV_WIDTH] = value_ref[...]
        out_ref[d, :, KV_WIDTH:] = down


def packed_shard(value_rows, down_rows, copies):
    return pl.pallas_call(
        pack_kernel,
        out_shape=jax.ShapeDtypeStruct((copies, RANK, WIDTH), jnp.bfloat16),
        compiler_params=pltpu.CompilerParams(vmem_limit_bytes=67_000_000),
        name="pack",
    )(value_rows, down_rows)


def places():
    place, plane = lax.axis_index("fsdp"), lax.axis_index("dp")
    return place & 1, (place >> 1) & 3, (plane & 1) * 2 + ((place >> 3) & 1)


def split_kernel(hidden, keep, send):
    first = lax.broadcasted_iota(jnp.int32, (TOK, HEAD_DIM), 1) < RANK
    mine = places()[0] == 0
    for x in range(4):
        for y in range(0, 8, 2):
            a = hidden[:, y * 512 + x * 128 : y * 512 + (x + 1) * 128].astype(jnp.float32)
            b = hidden[:, (y + 1) * 512 + x * 128 : (y + 1) * 512 + (x + 1) * 128].astype(jnp.float32)
            even = jnp.where(first, a, pltpu.roll(b, RANK, 1))
            odd = jnp.where(first, pltpu.roll(a, RANK, 1), b)
            to = pl.ds(x * 512 + y * 64, 128)
            keep[:, to] = jnp.where(mine, even, odd).astype(jnp.bfloat16)
            send[:, to] = jnp.where(mine, odd, even).astype(jnp.bfloat16)


def split_hidden(hidden):
    vmem = pl.BlockSpec(memory_space=pltpu.VMEM)
    shape = jax.ShapeDtypeStruct((TOK, MODEL // 2), jnp.bfloat16)
    return pl.pallas_call(
        split_kernel,
        in_specs=[vmem],
        out_specs=[vmem, vmem],
        out_shape=[shape, shape],
        compiler_params=pltpu.CompilerParams(vmem_limit_bytes=12 * 2**20),
        cost_estimate=pl.CostEstimate(flops=2**30, bytes_accessed=2**22, transcendentals=0),
        name="split",
    )(hidden)


def block_product(tokens, block, which):
    _, x, own_quarter = places()
    column = ((x + (4 - which)) & 3) * 512
    if len(block) == 1:
        return nn(tokens[:, pl.ds(pl.multiple_of(column, 512), 512)], block[0][...].reshape(512, WIDTH))
    total = None
    for j in (0, 2):
        left, right = [], []
        for k in (j, j + 1):
            quarter = own_quarter ^ k
            left.append(tokens[:, pl.ds(pl.multiple_of(column + quarter * 128, 128), 128)])
            right.append(block[k][...].reshape(128, WIDTH))
        part = nn(jnp.concatenate(left, axis=1), jnp.concatenate(right, axis=0))
        total = part if total is None else total + part
    return total


def first_kernel(mine, theirs, own, out):
    for i, tokens in enumerate((mine, theirs)):
        out[i] = block_product(tokens, (own,), 0)


def next_kernel(mine, theirs, far, before, out):
    for i, tokens in enumerate((mine, theirs)):
        out[i] = block_product(tokens, (far,), 3) + before[i]


def last_kernel(mine, theirs, q0, q1, q2, q3, near, before, own, other):
    for i, (tokens, out) in enumerate(((mine, own), (theirs, other))):
        far = block_product(tokens, (q0, q1, q2, q3), 2)
        out[:, :WIDTH] = (before[i] + far) + block_product(tokens, (near,), 1)
        out[:, WIDTH:] = jnp.zeros((TOK, PADDED - WIDTH), jnp.float32)


def partial_values(body, *given):
    vmem = pl.BlockSpec(memory_space=pltpu.VMEM)
    shape = jax.ShapeDtypeStruct
    last = body is last_kernel
    return pl.pallas_call(
        body,
        in_specs=[vmem] * len(given),
        out_specs=[vmem, vmem] if last else vmem,
        out_shape=[shape((TOK, PADDED), jnp.float32)] * 2 if last else shape((2, TOK, WIDTH), jnp.float32),
        compiler_params=pltpu.CompilerParams(vmem_limit_bytes=12 * 2**20),
        cost_estimate=pl.CostEstimate(flops=2**29, bytes_accessed=2**21, transcendentals=0),
        name="partial",
    )(*given)


def store_pieces(out_ref, latent_grad_t, hidden, up_term, facts, core):
    lane = lax.broadcasted_iota(jnp.int32, (RANK // 2, HEAD_DIM), 1) < RANK
    for x in range(4):
        term = nn(latent_grad_t, hidden[:, x * 512 : (x + 1) * 512])
        for i in range(4):
            a = term[: RANK // 2, i * 128 : (i + 1) * 128]
            b = term[RANK // 2 :, i * 128 : (i + 1) * 128]
            out_ref[8 * i + x, :32, :] = jnp.where(lane, a, pltpu.roll(b, RANK, 1))
            out_ref[8 * i + 4 + x, :32, :] = jnp.where(lane, pltpu.roll(a, RANK, 1), b)
    sub = lax.broadcasted_iota(jnp.int32, (8, HEAD_DIM), 0)
    for q in range(8):
        for b in range(4):
            tile = up_term[8 * q : 8 * q + 8, b * 128 : (b + 1) * 128]
            rows = jnp.where(core == 0, tile, pltpu.roll(tile, 4, 0))
            out_ref[4 * q + b, 32:, :] = jnp.where(sub < 4, rows, facts)


def grads_kernel(
    length_ref, hidden, before, swapped, probs, probs_t, target, up_ref,
    out_ref, latent_grad_ref, up_term_ref, sums_ref, cot, value_grad,
):
    length = length_ref[0]
    up = up_ref[...].astype(jnp.bfloat16)
    total = before[...] + swapped[...]
    latent = total[:, KV_WIDTH:WIDTH].astype(jnp.bfloat16)
    values = (total[:, :KV_WIDTH] + adapter_scale * nn(latent, up)).astype(jnp.bfloat16)

    live = lax.broadcasted_iota(jnp.int32, (TOK, HEAD_DIM), 0) < length
    squares = jnp.zeros((TOK, HEAD_DIM), jnp.float32)
    outputs = [nn(probs[k], values[:, k * HEAD_DIM : (k + 1) * HEAD_DIM]) for k in range(KEY_VALUE_HEADS)]
    for k in range(KEY_VALUE_HEADS):
        for g in range(GROUP):
            h = k * GROUP + g
            aim = target[:, h * HEAD_DIM : (h + 1) * HEAD_DIM].astype(jnp.float32)
            differ = jnp.where(live, outputs[k][g * TOK : (g + 1) * TOK, :] - aim, 0.0)
            squares = squares + differ * differ
            cot[k, g * TOK : (g + 1) * TOK, :] = differ.astype(jnp.bfloat16)
    for k in range(KEY_VALUE_HEADS):
        value_grad[:, k * HEAD_DIM : (k + 1) * HEAD_DIM] = nn(probs_t[k], cot[k]).astype(jnp.bfloat16)

    grad = value_grad[...]
    latent_grad_t = nt(up, grad).astype(jnp.bfloat16)
    up_term = lax.dot_general(latent, grad, (((0,), (0,)), ((), ())), preferred_element_type=jnp.float32)

    loss = jnp.sum(jnp.sum(squares, axis=0, keepdims=True), axis=1, keepdims=True)
    lane = lax.broadcasted_iota(jnp.int32, (8, HEAD_DIM), 1)
    row = lax.broadcasted_iota(jnp.int32, (8, HEAD_DIM), 0)
    count = jnp.full((8, HEAD_DIM), length, jnp.int32).astype(jnp.float32)
    sums = jnp.where(lane == 0, loss, jnp.where(lane == 1, count, 0.0))
    sums = jnp.where(row == 4, sums, 0.0)
    latent_grad_ref[...] = latent_grad_t
    up_term_ref[...] = up_term
    sums_ref[...] = sums
    store_pieces(out_ref, latent_grad_t, hidden, up_term, sums, 1 - places()[0])


PIECES = jax.ShapeDtypeStruct((MODEL // RANK // 2, PIECE_ROWS, HEAD_DIM), jnp.float32)


def gradients(lengths, hidden, before, swapped, probs, probs_t, target, up_map):
    vmem = pl.BlockSpec(memory_space=pltpu.VMEM)
    shape = jax.ShapeDtypeStruct
    return pl.pallas_call(
        grads_kernel,
        in_specs=[pl.BlockSpec(memory_space=pltpu.SMEM)] + [vmem] * 7,
        out_specs=[vmem] * 4,
        out_shape=[
            PIECES,
            shape((RANK, TOK), jnp.bfloat16),
            shape((RANK, KV_WIDTH), jnp.float32),
            shape((8, HEAD_DIM), jnp.float32),
        ],
        scratch_shapes=[
            pltpu.VMEM((KEY_VALUE_HEADS, GROUP * TOK, HEAD_DIM), jnp.bfloat16),
            pltpu.VMEM((TOK, KV_WIDTH), jnp.bfloat16),
        ],
        compiler_params=pltpu.CompilerParams(vmem_limit_bytes=24 * 2**20),
        cost_estimate=pl.CostEstimate(flops=2**32, bytes_accessed=10 * 2**20, transcendentals=0),
        name="grads",
    )(lengths, hidden, before, swapped, probs, probs_t, target, up_map)


def keep_kernel(hidden, latent_grad_ref, up_term_ref, sums_ref, out_ref):
    store_pieces(out_ref, latent_grad_ref[...], hidden, up_term_ref[...], sums_ref[...], places()[0])


def kept_pieces(hidden, latent_grad_t, up_term, sums):
    vmem = pl.BlockSpec(memory_space=pltpu.VMEM)
    return pl.pallas_call(
        keep_kernel,
        in_specs=[vmem] * 4,
        out_specs=vmem,
        out_shape=PIECES,
        compiler_params=pltpu.CompilerParams(vmem_limit_bytes=8 * 2**20),
        cost_estimate=pl.CostEstimate(flops=2**28, bytes_accessed=2**21, transcendentals=0),
        name="keep",
    )(hidden, latent_grad_t, up_term, sums)


def rounded(rows):
    row = lax.broadcasted_iota(jnp.int32, (8, HEAD_DIM), 0)
    rest = rows - rows.astype(jnp.bfloat16).astype(jnp.float32)
    return jnp.where(row == 5, pltpu.roll(rest, 1, 0), rows).astype(jnp.bfloat16)


def merge_kernel(kept, came, out_ref):
    for r in range(out_ref.shape[0]):
        out_ref[r, :32, :] = (kept[r, :32, :] + came[r, :32, :]).astype(jnp.bfloat16)
        out_ref[r, 32:, :] = rounded(kept[r, 32:, :] + came[r, 32:, :])


def merged(kept, came):
    return pl.pallas_call(
        merge_kernel,
        out_shape=jax.ShapeDtypeStruct(PIECES.shape, jnp.bfloat16),
        compiler_params=SMALL,
        name="merge",
    )(kept, came)


def fold_kernel(pieces_ref, out_ref):
    total = jnp.sum(pieces_ref[...].astype(jnp.float32), axis=0)
    row = lax.broadcasted_iota(jnp.int32, (8, HEAD_DIM), 0)
    tail = total[32:, :]
    tail = jnp.where(row == 4, tail + pltpu.roll(tail, 7, 0), tail)
    rows = jnp.concatenate([total[:32, :].astype(jnp.bfloat16), rounded(tail)], axis=0)
    for d in range(out_ref.shape[0]):
        out_ref[d] = rows


def fold(pieces, copies):
    return pl.pallas_call(
        fold_kernel,
        out_shape=jax.ShapeDtypeStruct((copies, PIECE_ROWS, HEAD_DIM), jnp.bfloat16),
        compiler_params=SMALL,
        name="fold",
    )(pieces)


def owner_kernel(pieces_ref, down_ref, average_ref, grad_ref, next_ref, up_ref, loss_ref):
    total = jnp.sum(pieces_ref[...].astype(jnp.float32), axis=0)
    sums = total[36:37, :] + total[37:38, :]
    count = sums[:, 1:2]
    loss_ref[...] = sums[:, 0:1] / (2.0 * count)
    factor = adapter_scale / count
    rows = jnp.concatenate([total[:32, :RANK], total[:32, RANK:]], axis=0)
    grad = jnp.transpose(rows) * factor
    grad_ref[...] = grad
    next_ref[...] = average_decay * average_ref[...] + (1.0 - average_decay) * (down_ref[...] - learning_rate * grad)
    piece = (total[32:36, :] * factor).astype(jnp.bfloat16)
    for d in range(up_ref.shape[0]):
        up_ref[d] = piece


def owner_update(pieces, down_map, average_down_map, copies):
    shape = jax.ShapeDtypeStruct
    return pl.pallas_call(
        owner_kernel,
        out_shape=[
            shape((RANK, RANK), jnp.float32),
            shape((RANK, RANK), jnp.float32),
            shape((copies, 4, HEAD_DIM), jnp.bfloat16),
            shape((1, 1), jnp.float32),
        ],
        compiler_params=SMALL,
        name="owner",
    )(pieces, down_map, average_down_map)


def second_kernel(pieces_ref, up_ref, average_ref, grad_ref, next_ref):
    for j in range(MODEL // RANK):
        q, b = divmod(j // 2, 4)
        top = 8 * q + 4 * (j % 2)
        grad_ref[top : top + 4, b * 128 : (b + 1) * 128] = pieces_ref[j].astype(jnp.float32)
    next_ref[...] = average_decay * average_ref[...] + (1.0 - average_decay) * (
        up_ref[...] - learning_rate * grad_ref[...]
    )


def second_update(pieces, up_map, average_up_map):
    shape = jax.ShapeDtypeStruct((RANK, KV_WIDTH), jnp.float32)
    return pl.pallas_call(second_kernel, out_shape=[shape, shape], compiler_params=SMALL, name="second")(
        pieces, up_map, average_up_map
    )


def exchange(pieces, axis):
    return lax.all_to_all(pieces, axis, 0, 0, tiled=True)


def along_y(owners):
    return [list(range(k, owners, 8)) for k in range(8)]


def same_core(owners):
    return [list(range(core, owners, 2)) for core in range(2)]


def along_x(block, owners, shift):
    moved = [(i, i // 8 * 8 + (i + 2 * shift) % 8) for i in range(owners)]
    return lax.ppermute(block, "fsdp", moved)


def from_neighbour(part, owners, replicas, y, z):
    moved = [
        ((d + z) % replicas * owners + (i + 8 * y) % owners, d * owners + i)
        for d in range(replicas)
        for i in range(owners)
    ]
    return lax.ppermute(part, ("dp", "fsdp"), moved)


def from_other_core(block, owners):
    return lax.ppermute(block, "fsdp", [(i, i ^ 1) for i in range(owners)])


def per_device(
    hidden,
    queries,
    keys,
    target,
    lengths,
    value_weight_frozen,
    adapter_down_map,
    adapter_up_map,
    average_down_map,
    average_up_map,
):
    owners, replicas = lax.axis_size("fsdp"), lax.axis_size("dp")
    quarter = places()[2]
    shards = packed_shard(value_weight_frozen, adapter_down_map, owners // 8)
    own = lax.all_to_all(shards, "fsdp", 0, 0, tiled=True, axis_index_groups=along_y(owners))
    mine, send = split_hidden(hidden)
    theirs = from_other_core(send, owners)
    probs, probs_t = attention_probs(lengths, queries, keys)
    part = along_x(lax.dynamic_slice_in_dim(own, quarter * 2, 2, axis=0), owners, 2)
    near = along_x(own, owners, 1)
    far = along_x(own, owners, 3)
    beside = from_neighbour(part, owners, replicas, 1, 0)
    behind = from_neighbour(part, owners, replicas, 0, 1)
    corner = from_neighbour(part, owners, replicas, 1, 1)
    total = partial_values(first_kernel, mine, theirs, own)
    total = partial_values(next_kernel, mine, theirs, far, total)
    total, other = partial_values(
        last_kernel, mine, theirs, part, beside, behind, corner, near, total
    )
    swapped = from_other_core(other, owners)
    pieces, latent_grad_t, up_term, sums = gradients(
        lengths, send, total, swapped, probs, probs_t, target, adapter_up_map
    )
    came = from_other_core(pieces, owners)
    kept = kept_pieces(mine, latent_grad_t, up_term, sums)
    arrived = lax.all_to_all(
        merged(kept, came), "fsdp", 0, 0, tiled=True, axis_index_groups=same_core(owners)
    )
    summed = fold(arrived, replicas)
    down_grad, average_down_next, up_piece, loss = owner_update(
        exchange(summed, "dp"), adapter_down_map, average_down_map, owners
    )
    up_grad, average_up_next = second_update(exchange(up_piece, "fsdp"), adapter_up_map, average_up_map)
    return (down_grad, up_grad, average_down_next, average_up_next, loss.reshape(()))


def solution(mesh):
    placed = (
        P(("dp", "fsdp"), None),
        P(("dp", "fsdp"), None),
        P(("dp", "fsdp"), None),
        P(("dp", "fsdp"), None),
        P(("dp", "fsdp")),
        P("fsdp", None),
        P("fsdp", None),
        P(),
        P("fsdp", None),
        P(),
    )
    return jax.shard_map(
        per_device,
        mesh=mesh,
        in_specs=placed,
        out_specs=(P("fsdp", None), P(), P("fsdp", None), P(), P()),
        check_vma=False,
    )
```

```python
import math

import jax
import jax.numpy as jnp
from jax import lax
from jax.experimental import pallas as pl
from jax.experimental.pallas import tpu as pltpu
from jax.sharding import PartitionSpec as P


HEADS = 16
KEY_VALUE_HEADS = 4
HEAD_DIM = 128
GROUP = HEADS // KEY_VALUE_HEADS
TOK = 256
MODEL = 4096
RANK = 64
KV_WIDTH = KEY_VALUE_HEADS * HEAD_DIM
WIDTH = KV_WIDTH + RANK
PADDED = KV_WIDTH + HEAD_DIM

adapter_scale = 2.0
average_decay = 0.9
learning_rate = 1.0
masked_score = -1e30

PIECE_ROWS = 40
SMALL = pltpu.CompilerParams(vmem_limit_bytes=4 * 2**20)


def nt(a, b):
    return lax.dot_general(a, b, (((1,), (1,)), ((), ())), preferred_element_type=jnp.float32)


def nn(a, b):
    return lax.dot_general(a, b, (((1,), (0,)), ((), ())), preferred_element_type=jnp.float32)


def probs_kernel(length_ref, q_ref, k_ref, p_ref, pt_ref):
    length = length_ref[0]
    keys = k_ref[...]
    row = lax.broadcasted_iota(jnp.int32, (TOK, TOK), 0)
    col = lax.broadcasted_iota(jnp.int32, (TOK, TOK), 1)
    allowed = (col <= row) & (col < length)
    for g in range(GROUP):
        scores = nt(q_ref[:, g * HEAD_DIM : (g + 1) * HEAD_DIM], keys) * (1.0 / math.sqrt(HEAD_DIM))
        scores = jnp.where(allowed, scores, masked_score)
        weights = jnp.exp(scores - jnp.max(scores, axis=-1, keepdims=True))
        probs = weights * (1.0 / jnp.sum(weights, axis=-1, keepdims=True))
        p_ref[0, g * TOK : (g + 1) * TOK, :] = probs.astype(jnp.bfloat16)
        pt_ref[0, :, g * TOK : (g + 1) * TOK] = jnp.transpose(probs).astype(jnp.bfloat16)


def attention_probs(lengths, queries, keys):
    shape = jax.ShapeDtypeStruct
    return pl.pallas_call(
        probs_kernel,
        grid=(KEY_VALUE_HEADS,),
        in_specs=[
            pl.BlockSpec(memory_space=pltpu.SMEM),
            pl.BlockSpec((TOK, GROUP * HEAD_DIM), lambda h: (0, h)),
            pl.BlockSpec((TOK, HEAD_DIM), lambda h: (0, h)),
        ],
        out_specs=[
            pl.BlockSpec((1, GROUP * TOK, TOK), lambda h: (h, 0, 0)),
            pl.BlockSpec((1, TOK, GROUP * TOK), lambda h: (h, 0, 0)),
        ],
        out_shape=[
            shape((KEY_VALUE_HEADS, GROUP * TOK, TOK), jnp.bfloat16),
            shape((KEY_VALUE_HEADS, TOK, GROUP * TOK), jnp.bfloat16),
        ],
        compiler_params=pltpu.CompilerParams(vmem_limit_bytes=60 * 2**20),
        cost_estimate=pl.CostEstimate(flops=2**31, bytes_accessed=6 * 2**20, transcendentals=2**20),
        name="probs",
    )(lengths, queries, keys)


def pack_kernel(value_ref, down_ref, out_ref):
    down = down_ref[...].astype(jnp.bfloat16)
    for d in range(out_ref.shape[0]):
        out_ref[d, :, :KV_WIDTH] = value_ref[...]
        out_ref[d, :, KV_WIDTH:] = down


def packed_shard(value_rows, down_rows, copies):
    return pl.pallas_call(
        pack_kernel,
        out_shape=jax.ShapeDtypeStruct((copies, RANK, WIDTH), jnp.bfloat16),
        compiler_params=pltpu.CompilerParams(vmem_limit_bytes=67_000_000),
        name="pack",
    )(value_rows, down_rows)


def places():
    place, plane = lax.axis_index("fsdp"), lax.axis_index("dp")
    return place & 1, (place >> 1) & 3, (plane & 1) * 2 + ((place >> 3) & 1)


def split_kernel(hidden, keep, send):
    first = lax.broadcasted_iota(jnp.int32, (TOK, HEAD_DIM), 1) < RANK
    mine = places()[0] == 0
    for x in range(4):
        for y in range(0, 8, 2):
            a = hidden[:, y * 512 + x * 128 : y * 512 + (x + 1) * 128].astype(jnp.float32)
            b = hidden[:, (y + 1) * 512 + x * 128 : (y + 1) * 512 + (x + 1) * 128].astype(jnp.float32)
            even = jnp.where(first, a, pltpu.roll(b, RANK, 1))
            odd = jnp.where(first, pltpu.roll(a, RANK, 1), b)
            to = pl.ds(x * 512 + y * 64, 128)
            keep[:, to] = jnp.where(mine, even, odd).astype(jnp.bfloat16)
            send[:, to] = jnp.where(mine, odd, even).astype(jnp.bfloat16)


def split_hidden(hidden):
    vmem = pl.BlockSpec(memory_space=pltpu.VMEM)
    shape = jax.ShapeDtypeStruct((TOK, MODEL // 2), jnp.bfloat16)
    return pl.pallas_call(
        split_kernel,
        in_specs=[vmem],
        out_specs=[vmem, vmem],
        out_shape=[shape, shape],
        compiler_params=pltpu.CompilerParams(vmem_limit_bytes=12 * 2**20),
        cost_estimate=pl.CostEstimate(flops=2**30, bytes_accessed=2**22, transcendentals=0),
        name="split",
    )(hidden)


def block_product(tokens, block, which):
    _, x, own_quarter = places()
    column = ((x + (4 - which)) & 3) * 512
    if len(block) == 1:
        return nn(tokens[:, pl.ds(pl.multiple_of(column, 512), 512)], block[0][...].reshape(512, WIDTH))
    total = None
    for j in (0, 2):
        left, right = [], []
        for k in (j, j + 1):
            quarter = own_quarter ^ k
            left.append(tokens[:, pl.ds(pl.multiple_of(column + quarter * 128, 128), 128)])
            right.append(block[k][...].reshape(128, WIDTH))
        part = nn(jnp.concatenate(left, axis=1), jnp.concatenate(right, axis=0))
        total = part if total is None else total + part
    return total


def first_kernel(mine, theirs, own, out):
    for i, tokens in enumerate((mine, theirs)):
        out[i] = block_product(tokens, (own,), 0)


def next_kernel(mine, theirs, far, before, out):
    for i, tokens in enumerate((mine, theirs)):
        out[i] = block_product(tokens, (far,), 3) + before[i]


def quarters_kernel(mine, theirs, q0, q1, q2, q3, before, out):
    for i, tokens in enumerate((mine, theirs)):
        out[i] = before[i] + block_product(tokens, (q0, q1, q2, q3), 2)


def last_kernel(mine, theirs, near, before, own, other):
    for i, (tokens, out) in enumerate(((mine, own), (theirs, other))):
        out[:, :WIDTH] = before[i] + block_product(tokens, (near,), 1)
        out[:, WIDTH:] = jnp.zeros((TOK, PADDED - WIDTH), jnp.float32)


def partial_values(body, *given):
    vmem = pl.BlockSpec(memory_space=pltpu.VMEM)
    shape = jax.ShapeDtypeStruct
    last = body is last_kernel
    return pl.pallas_call(
        body,
        in_specs=[vmem] * len(given),
        out_specs=[vmem, vmem] if last else vmem,
        out_shape=[shape((TOK, PADDED), jnp.float32)] * 2 if last else shape((2, TOK, WIDTH), jnp.float32),
        compiler_params=pltpu.CompilerParams(vmem_limit_bytes=12 * 2**20),
        cost_estimate=pl.CostEstimate(flops=2**29, bytes_accessed=2**21, transcendentals=0),
        name="partial",
    )(*given)


def store_pieces(out_ref, latent_grad_t, hidden, up_term, facts, core):
    lane = lax.broadcasted_iota(jnp.int32, (RANK // 2, HEAD_DIM), 1) < RANK
    for x in range(4):
        term = nn(latent_grad_t, hidden[:, x * 512 : (x + 1) * 512])
        for i in range(4):
            a = term[: RANK // 2, i * 128 : (i + 1) * 128]
            b = term[RANK // 2 :, i * 128 : (i + 1) * 128]
            out_ref[8 * i + x, :32, :] = jnp.where(lane, a, pltpu.roll(b, RANK, 1))
            out_ref[8 * i + 4 + x, :32, :] = jnp.where(lane, pltpu.roll(a, RANK, 1), b)
    sub = lax.broadcasted_iota(jnp.int32, (8, HEAD_DIM), 0)
    for q in range(8):
        for b in range(4):
            tile = up_term[8 * q : 8 * q + 8, b * 128 : (b + 1) * 128]
            rows = jnp.where(core == 0, tile, pltpu.roll(tile, 4, 0))
            out_ref[4 * q + b, 32:, :] = jnp.where(sub < 4, rows, facts)


def grads_kernel(
    length_ref, hidden, before, swapped, probs, probs_t, target, up_ref,
    out_ref, latent_grad_ref, up_term_ref, sums_ref, cot, value_grad,
):
    length = length_ref[0]
    up = up_ref[...].astype(jnp.bfloat16)
    total = before[...] + swapped[...]
    latent = total[:, KV_WIDTH:WIDTH].astype(jnp.bfloat16)
    values = (total[:, :KV_WIDTH] + adapter_scale * nn(latent, up)).astype(jnp.bfloat16)

    live = lax.broadcasted_iota(jnp.int32, (TOK, HEAD_DIM), 0) < length
    squares = jnp.zeros((TOK, HEAD_DIM), jnp.float32)
    outputs = [nn(probs[k], values[:, k * HEAD_DIM : (k + 1) * HEAD_DIM]) for k in range(KEY_VALUE_HEADS)]
    for k in range(KEY_VALUE_HEADS):
        for g in range(GROUP):
            h = k * GROUP + g
            aim = target[:, h * HEAD_DIM : (h + 1) * HEAD_DIM].astype(jnp.float32)
            differ = jnp.where(live, outputs[k][g * TOK : (g + 1) * TOK, :] - aim, 0.0)
            squares = squares + differ * differ
            cot[k, g * TOK : (g + 1) * TOK, :] = differ.astype(jnp.bfloat16)
    for k in range(KEY_VALUE_HEADS):
        value_grad[:, k * HEAD_DIM : (k + 1) * HEAD_DIM] = nn(probs_t[k], cot[k]).astype(jnp.bfloat16)

    grad = value_grad[...]
    latent_grad_t = nt(up, grad).astype(jnp.bfloat16)
    up_term = lax.dot_general(latent, grad, (((0,), (0,)), ((), ())), preferred_element_type=jnp.float32)

    loss = jnp.sum(jnp.sum(squares, axis=0, keepdims=True), axis=1, keepdims=True)
    lane = lax.broadcasted_iota(jnp.int32, (8, HEAD_DIM), 1)
    row = lax.broadcasted_iota(jnp.int32, (8, HEAD_DIM), 0)
    count = jnp.full((8, HEAD_DIM), length, jnp.int32).astype(jnp.float32)
    sums = jnp.where(lane == 0, loss, jnp.where(lane == 1, count, 0.0))
    sums = jnp.where(row == 4, sums, 0.0)
    latent_grad_ref[...] = latent_grad_t
    up_term_ref[...] = up_term
    sums_ref[...] = sums
    store_pieces(out_ref, latent_grad_t, hidden, up_term, sums, 1 - places()[0])


PIECES = jax.ShapeDtypeStruct((MODEL // RANK // 2, PIECE_ROWS, HEAD_DIM), jnp.float32)


def gradients(lengths, hidden, before, swapped, probs, probs_t, target, up_map):
    vmem = pl.BlockSpec(memory_space=pltpu.VMEM)
    shape = jax.ShapeDtypeStruct
    return pl.pallas_call(
        grads_kernel,
        in_specs=[pl.BlockSpec(memory_space=pltpu.SMEM)] + [vmem] * 7,
        out_specs=[vmem] * 4,
        out_shape=[
            PIECES,
            shape((RANK, TOK), jnp.bfloat16),
            shape((RANK, KV_WIDTH), jnp.float32),
            shape((8, HEAD_DIM), jnp.float32),
        ],
        scratch_shapes=[
            pltpu.VMEM((KEY_VALUE_HEADS, GROUP * TOK, HEAD_DIM), jnp.bfloat16),
            pltpu.VMEM((TOK, KV_WIDTH), jnp.bfloat16),
        ],
        compiler_params=pltpu.CompilerParams(vmem_limit_bytes=24 * 2**20),
        cost_estimate=pl.CostEstimate(flops=2**32, bytes_accessed=10 * 2**20, transcendentals=0),
        name="grads",
    )(lengths, hidden, before, swapped, probs, probs_t, target, up_map)


def keep_kernel(hidden, latent_grad_ref, up_term_ref, sums_ref, out_ref):
    store_pieces(out_ref, latent_grad_ref[...], hidden, up_term_ref[...], sums_ref[...], places()[0])


def kept_pieces(hidden, latent_grad_t, up_term, sums):
    vmem = pl.BlockSpec(memory_space=pltpu.VMEM)
    return pl.pallas_call(
        keep_kernel,
        in_specs=[vmem] * 4,
        out_specs=vmem,
        out_shape=PIECES,
        compiler_params=pltpu.CompilerParams(vmem_limit_bytes=8 * 2**20),
        cost_estimate=pl.CostEstimate(flops=2**28, bytes_accessed=2**21, transcendentals=0),
        name="keep",
    )(hidden, latent_grad_t, up_term, sums)


def rounded(rows):
    row = lax.broadcasted_iota(jnp.int32, (8, HEAD_DIM), 0)
    rest = rows - rows.astype(jnp.bfloat16).astype(jnp.float32)
    return jnp.where(row == 5, pltpu.roll(rest, 1, 0), rows).astype(jnp.bfloat16)


def merge_kernel(kept, came, out_ref):
    for r in range(out_ref.shape[0]):
        out_ref[r, :32, :] = (kept[r, :32, :] + came[r, :32, :]).astype(jnp.bfloat16)
        out_ref[r, 32:, :] = rounded(kept[r, 32:, :] + came[r, 32:, :])


def merged(kept, came):
    return pl.pallas_call(
        merge_kernel,
        out_shape=jax.ShapeDtypeStruct(PIECES.shape, jnp.bfloat16),
        compiler_params=SMALL,
        name="merge",
    )(kept, came)


def fold_kernel(pieces_ref, out_ref):
    total = jnp.sum(pieces_ref[...].astype(jnp.float32), axis=0)
    row = lax.broadcasted_iota(jnp.int32, (8, HEAD_DIM), 0)
    tail = total[32:, :]
    tail = jnp.where(row == 4, tail + pltpu.roll(tail, 7, 0), tail)
    rows = jnp.concatenate([total[:32, :].astype(jnp.bfloat16), rounded(tail)], axis=0)
    for d in range(out_ref.shape[0]):
        out_ref[d] = rows


def fold(pieces, copies):
    return pl.pallas_call(
        fold_kernel,
        out_shape=jax.ShapeDtypeStruct((copies, PIECE_ROWS, HEAD_DIM), jnp.bfloat16),
        compiler_params=SMALL,
        name="fold",
    )(pieces)


def owner_kernel(pieces_ref, down_ref, average_ref, grad_ref, next_ref, up_ref, loss_ref):
    total = jnp.sum(pieces_ref[...].astype(jnp.float32), axis=0)
    sums = total[36:37, :] + total[37:38, :]
    count = sums[:, 1:2]
    loss_ref[...] = sums[:, 0:1] / (2.0 * count)
    factor = adapter_scale / count
    rows = jnp.concatenate([total[:32, :RANK], total[:32, RANK:]], axis=0)
    grad = jnp.transpose(rows) * factor
    grad_ref[...] = grad
    next_ref[...] = average_decay * average_ref[...] + (1.0 - average_decay) * (down_ref[...] - learning_rate * grad)
    piece = (total[32:36, :] * factor).astype(jnp.bfloat16)
    for d in range(up_ref.shape[0]):
        up_ref[d] = piece


def owner_update(pieces, down_map, average_down_map, copies):
    shape = jax.ShapeDtypeStruct
    return pl.pallas_call(
        owner_kernel,
        out_shape=[
            shape((RANK, RANK), jnp.float32),
            shape((RANK, RANK), jnp.float32),
            shape((copies, 4, HEAD_DIM), jnp.bfloat16),
            shape((1, 1), jnp.float32),
        ],
        compiler_params=SMALL,
        name="owner",
    )(pieces, down_map, average_down_map)


def second_kernel(pieces_ref, up_ref, average_ref, grad_ref, next_ref):
    for j in range(MODEL // RANK):
        q, b = divmod(j // 2, 4)
        top = 8 * q + 4 * (j % 2)
        grad_ref[top : top + 4, b * 128 : (b + 1) * 128] = pieces_ref[j].astype(jnp.float32)
    next_ref[...] = average_decay * average_ref[...] + (1.0 - average_decay) * (
        up_ref[...] - learning_rate * grad_ref[...]
    )


def second_update(pieces, up_map, average_up_map):
    shape = jax.ShapeDtypeStruct((RANK, KV_WIDTH), jnp.float32)
    return pl.pallas_call(second_kernel, out_shape=[shape, shape], compiler_params=SMALL, name="second")(
        pieces, up_map, average_up_map
    )


def exchange(pieces, axis):
    return lax.all_to_all(pieces, axis, 0, 0, tiled=True)


def along_y(owners):
    return [list(range(k, owners, 8)) for k in range(8)]


def same_core(owners):
    return [list(range(core, owners, 2)) for core in range(2)]


def along_x(block, owners, shift):
    moved = [(i, i // 8 * 8 + (i + 2 * shift) % 8) for i in range(owners)]
    return lax.ppermute(block, "fsdp", moved)


def from_neighbour(part, owners, replicas, y, z):
    moved = [
        ((d + z) % replicas * owners + (i + 8 * y) % owners, d * owners + i)
        for d in range(replicas)
        for i in range(owners)
    ]
    return lax.ppermute(part, ("dp", "fsdp"), moved)


def from_other_core(block, owners):
    return lax.ppermute(block, "fsdp", [(i, i ^ 1) for i in range(owners)])


def per_device(
    hidden,
    queries,
    keys,
    target,
    lengths,
    value_weight_frozen,
    adapter_down_map,
    adapter_up_map,
    average_down_map,
    average_up_map,
):
    owners, replicas = lax.axis_size("fsdp"), lax.axis_size("dp")
    quarter = places()[2]
    shards = packed_shard(value_weight_frozen, adapter_down_map, owners // 8)
    own = lax.all_to_all(shards, "fsdp", 0, 0, tiled=True, axis_index_groups=along_y(owners))
    mine, send = split_hidden(hidden)
    theirs = from_other_core(send, owners)
    probs, probs_t = attention_probs(lengths, queries, keys)
    part = along_x(lax.dynamic_slice_in_dim(own, quarter * 2, 2, axis=0), owners, 2)
    near = along_x(own, owners, 1)
    far = along_x(own, owners, 3)
    beside = from_neighbour(part, owners, replicas, 1, 0)
    behind = from_neighbour(part, owners, replicas, 0, 1)
    corner = from_neighbour(part, owners, replicas, 1, 1)
    total = partial_values(first_kernel, mine, theirs, own)
    total = partial_values(next_kernel, mine, theirs, far, total)
    total = partial_values(quarters_kernel, mine, theirs, part, beside, behind, corner, total)
    total, other = partial_values(last_kernel, mine, theirs, near, total)
    swapped = from_other_core(other, owners)
    pieces, latent_grad_t, up_term, sums = gradients(
        lengths, send, total, swapped, probs, probs_t, target, adapter_up_map
    )
    came = from_other_core(pieces, owners)
    kept = kept_pieces(mine, latent_grad_t, up_term, sums)
    arrived = lax.all_to_all(
        merged(kept, came), "fsdp", 0, 0, tiled=True, axis_index_groups=same_core(owners)
    )
    summed = fold(arrived, replicas)
    down_grad, average_down_next, up_piece, loss = owner_update(
        exchange(summed, "dp"), adapter_down_map, average_down_map, owners
    )
    up_grad, average_up_next = second_update(exchange(up_piece, "fsdp"), adapter_up_map, average_up_map)
    return (down_grad, up_grad, average_down_next, average_up_next, loss.reshape(()))


def solution(mesh):
    placed = (
        P(("dp", "fsdp"), None),
        P(("dp", "fsdp"), None),
        P(("dp", "fsdp"), None),
        P(("dp", "fsdp"), None),
        P(("dp", "fsdp")),
        P("fsdp", None),
        P("fsdp", None),
        P(),
        P("fsdp", None),
        P(),
    )
    return jax.shard_map(
        per_device,
        mesh=mesh,
        in_specs=placed,
        out_specs=(P("fsdp", None), P(), P("fsdp", None), P(), P()),
        check_vma=False,
    )
```
